32 devices in a mesh: grp: 2 (over y), zt: 4 (over x, core), xy: 4 (over z).
Axes of the slice: x: 2, y: 2, z: 4, core: 2. Of those that a mesh axis runs over, the one named last changes fastest.
Arguments:
- source: float32 [2, 2, 3, 8, 16, 128], P('grp', None, None, 'xy', 'zt'), may hold values from -6 to 6
- links: float32 [4, 2, 3, 3, 8, 16, 128], P('grp', None, None, None, 'xy', 'zt'), may hold values from -2 to 2
- shifts: float32 [12], replicated, may hold values from 0.01 to 0.5
- residues: float32 [12], replicated, may hold values from 0.05 to 0.5
- mass: float32 [1], replicated, may hold values from 0.1 to 0.5
Outputs:
- rational: float32 [2, 2, 3, 8, 16, 128], P('grp', None, None, 'xy', 'zt')
- action: float32 [1], replicated
The draws below stay inside these ranges and needn't reach their ends.
All inputs are finite; a program needn't handle non-finite values.
Results may differ from the reference program's by a relative error of at most 0.0003.
Values sent between devices are 32-bit elements; how exact they have to be, the bound alone decides.
A program may use at most 64 MiB of HBM per device.

```python
import math
import jax
import jax.numpy as jnp

NY = 2
NZ = 64
NSHIFT = 12
ITERS = 8
PF = 2
NX = 8
NT = 16


def levels(own_key, extent, split, smallest, high):
    def one(position, shards_of):
        draws = jax.random.uniform(jax.random.fold_in(jax.random.fold_in(own_key, 6), position), (shards_of,), jnp.float32, smallest / len(split), high / len(split))
        return jnp.repeat(jnp.exp(draws), extent[position] // shards_of).reshape((-1,) + (1,) * (len(extent) - position - 1))

    gain = one(*split[0])
    for cut in split[1:]:
        gain = gain * one(*cut)
    return gain


def centred(own_key, dims, width, bound, cuts=(), held_as=jnp.bfloat16):
    result = width * jax.random.normal(own_key, dims, jnp.float32)
    if cuts:
        result = result * levels(own_key, dims, cuts, -0.22, 0.18)
    return jnp.clip(result, -bound, bound).astype(held_as)


def setup_inputs(seed: int = 0) -> dict:
    key_of = jax.random.split(jax.random.key(seed), 6)
    return {
        "source": centred(key_of[0], (PF, 2, 3, NX, NT, NY * NZ), 1.0, 6.0, ((0, 2), (3, 4), (4, 4)), jnp.float32),
        "links": centred(key_of[1], (4, 2, 3, 3, NX, NT, NY * NZ), 0.35, 2.0, ((0, 2), (4, 4), (5, 4)), jnp.float32),
        "shifts": jnp.clip(jnp.exp(jax.random.uniform(key_of[2], (NSHIFT,), jnp.float32, math.log(0.01), math.log(0.5))), 0.01, 0.5),
        "residues": jnp.clip(jnp.exp(jax.random.uniform(key_of[3], (NSHIFT,), jnp.float32, math.log(0.05), math.log(0.5))), 0.05, 0.5),
        "mass": jnp.clip(jnp.exp(jax.random.uniform(key_of[4], (1,), jnp.float32, math.log(0.1), math.log(0.5))), 0.1, 0.5),
    }


def sign_of(values):
    return (1 - 2 * (values % 2)).astype(jnp.float32)


def phases(coord_x, coord_t, last_t):
    yz_index = jnp.arange(NY * NZ, dtype=jnp.int32)
    ycoord = yz_index // NZ
    zcoord = yz_index % NZ
    unity = jnp.ones((coord_x.shape[0], coord_t.shape[0], NY * NZ), jnp.float32)
    boundary = jnp.where(coord_t == last_t, -1.0, 1.0).astype(jnp.float32)
    eta_y = sign_of(coord_x)[:, None, None] * unity
    eta_z = sign_of(coord_x[:, None, None] + ycoord[None, None, :]) * unity
    eta_t = sign_of(coord_x[:, None, None] + ycoord[None, None, :] + zcoord[None, None, :]) * boundary[None, :, None]
    return jnp.stack([unity, eta_y, eta_z, eta_t])


def times_link(link, field):
    real = jnp.sum(link[0][None] * field[:, 0][:, None] - link[1][None] * field[:, 1][:, None], axis=2)
    imag = jnp.sum(link[0][None] * field[:, 1][:, None] + link[1][None] * field[:, 0][:, None], axis=2)
    return jnp.stack([real, imag], axis=1)


def times_adjoint(link, field):
    real = jnp.sum(link[0][None] * field[:, 0][:, :, None] + link[1][None] * field[:, 1][:, :, None], axis=1)
    imag = jnp.sum(link[0][None] * field[:, 1][:, :, None] - link[1][None] * field[:, 0][:, :, None], axis=1)
    return jnp.stack([real, imag], axis=1)


def roll_ycoord(values, offset):
    return jnp.roll(values, offset * NZ, axis=-1)


def roll_zcoord(values, offset):
    shape = values.shape
    return jnp.roll(values.reshape(shape[:-1] + (NY, NZ)), offset, axis=-1).reshape(shape)


def hopping(field, folded):
    total = times_link(folded[0], jnp.roll(field, -1, axis=3)) - jnp.roll(times_adjoint(folded[0], field), 1, axis=3)
    total = total + times_link(folded[1], roll_ycoord(field, -1)) - roll_ycoord(times_adjoint(folded[1], field), 1)
    total = total + times_link(folded[2], roll_zcoord(field, -1)) - roll_zcoord(times_adjoint(folded[2], field), 1)
    total = total + times_link(folded[3], jnp.roll(field, -1, axis=4)) - jnp.roll(times_adjoint(folded[3], field), 1, axis=4)
    return 0.5 * total


def local_dot(left, right):
    return jnp.sum(left * right, axis=(1, 2, 3, 4, 5))


def spread(values):
    return values.reshape(values.shape + (1, 1, 1, 1, 1))


def rational_of(source, apply_normal, shifts, residues):
    shift_col = shifts[:, None]
    members = source.shape[0]
    residual = source
    direction = source
    solutions = jnp.zeros((shifts.shape[0],) + source.shape, jnp.float32)
    directions = jnp.broadcast_to(source[None], solutions.shape)
    norm_now = local_dot(source, source)
    zeta_now = jnp.ones((shifts.shape[0], members), jnp.float32)
    zeta_old = jnp.ones((shifts.shape[0], members), jnp.float32)
    alpha_old = jnp.ones((members,), jnp.float32)
    beta_old = jnp.zeros((members,), jnp.float32)
    for iteration in range(ITERS):
        image = apply_normal(direction)
        alpha_now = norm_now / local_dot(direction, image)
        zeta_new = zeta_now * zeta_old * alpha_old / (alpha_now * beta_old * (zeta_old - zeta_now) + zeta_old * alpha_old * (1.0 + shift_col * alpha_now))
        alpha_shift = alpha_now * zeta_new / zeta_now
        solutions = solutions + spread(alpha_shift) * directions
        if iteration + 1 < ITERS:
            residual = residual - spread(alpha_now) * image
            norm_next = local_dot(residual, residual)
            beta_now = norm_next / norm_now
            beta_shift = beta_now * (zeta_new / zeta_now) ** 2
            direction = residual + spread(beta_now) * direction
            directions = spread(zeta_new) * residual[None] + spread(beta_shift) * directions
            zeta_old = zeta_now
            zeta_now = zeta_new
            alpha_old = alpha_now
            beta_old = beta_now
            norm_now = norm_next
    return jnp.sum(residues.reshape((-1, 1, 1, 1, 1, 1, 1)) * solutions, axis=0)


def reference(source, links, shifts, residues, mass):
    eta = phases(jnp.arange(NX, dtype=jnp.int32), jnp.arange(NT, dtype=jnp.int32), NT - 1)
    folded = links * eta[:, None, None, None]
    mass_sq = mass[0] * mass[0]

    def apply_normal(field):
        return mass_sq * field - hopping(hopping(field, folded), folded)

    pieces = []
    for member in range(PF):
        pieces.append(rational_of(source[member:member + 1], apply_normal, shifts, residues))
    rational = jnp.concatenate(pieces, axis=0)
    action = (jnp.sum(source * rational) / (PF * NX * NT * NY * NZ)).reshape(1)
    return rational, action
```

```python
import functools

import jax
import jax.numpy as jnp
from jax import lax
from jax.experimental import pallas as pl
from jax.experimental.pallas import tpu as pltpu
from jax.sharding import PartitionSpec as P

NY = 2
NZ = 64
ITERS = 8
PAIRS = 9
MAT = 2 * PAIRS
COMPS = 6


def roll(value, shift, axis):
    size = value.shape[axis]
    return pltpu.roll(value, shift % size, axis)


def kernel(
    dims, source_hbm, links_hbm, shifts_hbm, residues_hbm, mass_hbm, out_ref, action_ref,
    lk, tfar, xfar, xtwo, sx, st, sx2, cs_ll, cs_hl, cs_lh, c_ll, c_hl, c_lh,
    gauge, dirn, resid, mid, shiftdirs, rpack, ws, cs, hb, part, cross,
    state, mine, theirs, source_ref, links_ref, shifts_ref, residues_ref, mass_ref,
    isem, lsend, lrecv, hsend, hrecv, psend, precv, asend, arecv,
):
    n_grp, n_zt, n_xy, cells_x, cells_t = dims
    lanes = NY * NZ
    n_all = n_zt * n_xy
    nshift = shifts_ref.shape[0]
    g = lax.axis_index("grp")
    zt = lax.axis_index("zt")
    xy = lax.axis_index("xy")
    me = zt * n_xy + xy
    me_all = g * n_all + me
    x_up, x_dn = lax.rem(xy + 1, n_xy), lax.rem(xy + n_xy - 1, n_xy)
    t_up, t_dn = lax.rem(zt + 1, n_zt), lax.rem(zt + n_zt - 1, n_zt)
    other = 1 - g

    def place(linear):
        inside = lax.rem(linear, n_all)
        return (linear // n_all, inside // n_xy, lax.rem(inside, n_xy))

    def each(count, fn):
        if count <= 32:
            for p in range(1, count):
                fn(p)
        else:
            def step(p, carry):
                fn(p)
                return carry
            lax.fori_loop(1, count, step, 0)

    def copy(src, dst, send, recv, device):
        return pltpu.make_async_remote_copy(
            src_ref=src, dst_ref=dst, send_sem=send, recv_sem=recv,
            device_id=device, device_id_type=pl.DeviceIdType.MESH,
        )

    barrier = pltpu.get_barrier_semaphore()

    def greet(p):
        pl.semaphore_signal(
            barrier, inc=1, device_id=place(lax.rem(me_all + p, n_grp * n_all)),
            device_id_type=pl.DeviceIdType.MESH,
        )

    fetch_links = pltpu.make_async_copy(links_hbm, links_ref, isem.at[0])
    fetch_source = pltpu.make_async_copy(source_hbm, source_ref, isem.at[1])
    each(n_grp * n_all, greet)
    fetch_links.start()
    fetch_source.start()
    scalars = [
        pltpu.make_async_copy(src, dst, isem.at[2 + k])
        for k, (src, dst) in enumerate(((shifts_hbm, shifts_ref), (residues_hbm, residues_ref), (mass_hbm, mass_ref)))
    ]
    for item in scalars:
        item.start()
    fetch_links.wait()
    fetch_source.wait()

    sub = lax.broadcasted_iota(jnp.int32, (8, lanes), 0)
    lane = lax.broadcasted_iota(jnp.int32, (8, lanes), 1)
    zcoord = lax.rem(lane, NZ)
    ycoord = lane // NZ
    quarter = lanes // 4
    home = sub == lane // quarter
    own = (sub >= 2) & (sub < 2 + cells_t)
    first = sub < cells_t
    late = lax.rem(sub, cells_t) >= 2

    def t_faces(c, one, two):
        st[0, pl.ds(c, 1)] = jnp.where(late, one, roll(two, -2, 0))[None]
        st[1, pl.ds(c, 1)] = jnp.where(late, roll(two, 2, 0), one)[None]

    for d in range(2):
        for c in range(MAT):
            low, high = links_ref[c], links_ref[MAT + c]
            if d == 0:
                sx[0, pl.ds(g * MAT + c, 1)] = jnp.where(first, roll(low, 4, 0), high)[None]
            else:
                sx[1, pl.ds(g * MAT + c, 1)] = jnp.where(first, low, roll(high, 4, 0))[None]
    for c in range(MAT):
        t_faces(g * MAT + c, links_ref[c], links_ref[MAT + c])
    for c in range(2 * MAT):
        lk[pl.ds(g * 2 * MAT + c, 1)] = links_ref[c][None]

    spack = [source_ref[c] for c in range(COMPS)]

    def corner_tiles(tiles, par):
        for k, row in enumerate((7, 4, 3, 0)):
            tile = jnp.zeros((8, lanes), jnp.float32)
            for c in range(COMPS):
                tile = jnp.where(sub == c, jnp.broadcast_to(tiles[c][row:row + 1], (8, lanes)), tile)
            cs[par, k] = tile

    corner_dev = ((g, t_up, x_up), (g, t_dn, x_up), (g, t_up, x_dn), (g, t_dn, x_dn))

    def halo(par):
        routes = ((g, zt, x_up), (g, zt, x_dn), (g, t_up, xy), (g, t_dn, xy))
        found = []
        for k in range(4):
            found.append(copy(cs.at[par, pl.ds(k, 1)], hb.at[par, pl.ds(4 * COMPS + k, 1)], hsend.at[par], hrecv.at[par], corner_dev[k]))
        for k in range(4):
            found.append(copy(ws.at[par], hb.at[par, pl.ds(k * COMPS, COMPS)], hsend.at[par], hrecv.at[par], routes[k]))
        return found

    def send_part(par):
        def go(p):
            copy(part.at[par, me], part.at[par, me], psend.at[par], precv.at[par],
                 (g,) + place(lax.rem(me + p, n_all))[1:]).start()
        each(n_all, go)

    def wait_part(par):
        rest = part.at[par, pl.ds(0, n_all - 1)]
        copy(rest, rest, psend.at[par], precv.at[par], corner_dev[0]).wait()

    def send_cross(par):
        def go(p):
            copy(part.at[par, me], cross.at[me], asend.at[0], arecv.at[0],
                 (other,) + place(lax.rem(me + p, n_all))[1:]).start()
        go(0)
        each(n_all, go)

    def dots(rows):
        tile = jnp.zeros((8, lanes), jnp.float32)
        for k, row in enumerate(rows):
            tile = jnp.where(sub == k, jnp.broadcast_to(jnp.sum(row, axis=0, keepdims=True), (8, lanes)), tile)
        tile = tile + roll(tile, 2 * quarter, 1)
        tile = tile + roll(tile, quarter, 1)
        return jnp.sum(jnp.where(home, tile, 0.0), axis=0, keepdims=True)

    def summed(row_of):
        if n_all <= 32:
            level = [row_of(j) for j in range(n_all)]
            while len(level) > 1:
                odd = level[len(level) // 2 * 2:]
                level = [level[k] + level[k + 1] for k in range(0, len(level) - 1, 2)] + odd
            total = level[0]
        else:
            total = lax.fori_loop(1, n_all, lambda j, acc: acc + row_of(j), row_of(0))
        split = jnp.where(home, jnp.broadcast_to(total, (8, lanes)), 0.0)
        return jnp.broadcast_to(jnp.sum(split, axis=1, keepdims=True), (8, lanes))

    def fill(values, k):
        return jnp.broadcast_to(values[k:k + 1], (16, lanes))

    def inner(left, right):
        total = left[0] * right[0]
        for c in range(1, COMPS):
            total = total + left[c] * right[c]
        return total

    corner_tiles(spack, 0)
    for c in range(COMPS):
        ws[0, c] = spack[c]
    part[0, pl.ds(me, 1)] = dots([inner(spack, spack)])[None]

    pl.semaphore_wait(barrier, n_grp * n_all - 1)

    half = 2 * MAT
    to_pair = copy(links_ref, lk.at[pl.ds(g * half, half)], lsend.at[0], lrecv.at[0], (other, zt, xy))
    to_pair.start()

    def link_faces(h):
        span = pl.ds(h * MAT, MAT)
        return [
            copy(sx.at[0, span], xfar.at[0, span], lsend.at[1], lrecv.at[1], (g, zt, x_up)),
            copy(sx.at[1, span], xfar.at[1, span], lsend.at[1], lrecv.at[1], (g, zt, x_dn)),
            copy(st.at[0, span], tfar.at[0, span], lsend.at[2], lrecv.at[2], (g, t_up, xy)),
            copy(st.at[1, span], tfar.at[1, span], lsend.at[2], lrecv.at[2], (g, t_dn, xy)),
        ]

    for item in link_faces(g):
        item.start()
    send_part(0)
    for item in halo(0):
        item.start()

    to_pair.wait_recv()
    for c in range(MAT):
        low, high = lk[other * half + c], lk[other * half + MAT + c]
        sx[0, pl.ds(other * MAT + c, 1)] = jnp.where(first, roll(low, 4, 0), high)[None]
        sx[1, pl.ds(other * MAT + c, 1)] = jnp.where(first, low, roll(high, 4, 0))[None]
        t_faces(other * MAT + c, low, high)
    for c in range(PAIRS):
        sx2[c] = jnp.where(first, lk[c], roll(lk[PAIRS + c], 4, 0))
    for c in range(MAT):
        cs_ll[c:c + 1] = lk[c][7:8]
        cs_ll[MAT + c:MAT + c + 1] = lk[3 * MAT + c][7:8]
        cs_hl[c:c + 1] = lk[3 * MAT + c][3:4]
        cs_lh[c:c + 1] = lk[c][4:5]
    rest = [
        copy(sx2, xtwo, lsend.at[3], lrecv.at[3], (g, zt, x_up)),
        copy(cs_ll, c_ll, lsend.at[4], lrecv.at[4], corner_dev[0]),
        copy(cs_hl, c_hl, lsend.at[5], lrecv.at[5], corner_dev[2]),
        copy(cs_lh, c_lh, lsend.at[6], lrecv.at[6], corner_dev[1]),
    ]
    for item in rest + link_faces(other):
        item.start()

    def pick(ref, c):
        return jnp.broadcast_to(ref[c:c + 1], (8, lanes))

    def widen(c, x, mine, low, high):
        between = jnp.where(late, low, high)
        return jnp.where(own, roll(mine, 2 - 4 * x, 0), roll(between, 6 - 4 * x, 0))

    def far_rows(block, low_corner, high_corner, x):
        row = jnp.where(own, roll(block, 2 - 4 * x, 0), 0.0)
        if low_corner is not None:
            row = jnp.where(sub == 1, low_corner, row)
        if high_corner is not None:
            row = jnp.where(sub == 6, high_corner, row)
        return row

    def extend(par, c):
        own_part = ws[par, c]
        corner = [jnp.broadcast_to(hb[par, 4 * COMPS + k, c:c + 1], (8, lanes)) for k in range(4)]
        x_lo, x_hi, t_lo, t_hi = [hb[par, k * COMPS + c] for k in range(4)]
        return [
            far_rows(x_lo, None, None, 0),
            far_rows(x_lo, corner[0], corner[1], 1),
            widen(c, 0, own_part, t_lo, t_hi),
            widen(c, 1, own_part, t_lo, t_hi),
            far_rows(x_hi, corner[2], corner[3], 0),
            far_rows(x_hi, None, None, 1),
        ]

    for item in scalars:
        item.wait()
    rows16 = lax.broadcasted_iota(jnp.int32, (16, lanes), 0)
    shift_rows = jnp.zeros((16, lanes), jnp.float32)
    residue_rows = jnp.zeros((16, lanes), jnp.float32)
    for k in range(nshift):
        shift_rows = jnp.where(rows16 == k, shifts_ref[k], shift_rows)
        residue_rows = jnp.where(rows16 == k, residues_ref[k], residue_rows)
    mass_sq = mass_ref[0] * mass_ref[0]

    for c in range(COMPS):
        rpack[c] = spack[c]
        out_ref[c] = jnp.zeros((8, lanes), jnp.float32)
        for k in range(nshift):
            shiftdirs[k, c] = spack[c]

    copy(st, tfar, lsend.at[2], lrecv.at[2], (g, t_up, xy)).wait()
    to_pair.wait_send()

    t_at = lax.rem(zt * cells_t + sub - 2 + n_zt * cells_t, n_zt * cells_t)
    edge = jnp.where(t_at == n_zt * cells_t - 1, -0.5, 0.5)
    yz_sign = (1 - 2 * lax.rem(ycoord + zcoord, 2)).astype(jnp.float32)
    y_sign = (1 - 2 * lax.rem(ycoord, 2)).astype(jnp.float32)

    def z_up(v):
        cond = jnp.broadcast_to(zcoord == NZ - 1, v.shape)
        return jnp.where(cond, roll(v, NZ - 1, v.ndim - 1), roll(v, -1, v.ndim - 1))

    def z_dn(v):
        cond = jnp.broadcast_to(zcoord == 0, v.shape)
        return jnp.where(cond, roll(v, 1 - NZ, v.ndim - 1), roll(v, 1, v.ndim - 1))

    def wide_link(d, c, e):
        at = d * MAT + c
        sign = -1.0 if e % 2 else 1.0
        if e in (2, 3):
            low, high = tfar[0, (d // 2) * MAT + c], tfar[1, (d // 2) * MAT + c]
            if d % 2:
                low, high = roll(low, 2, 0), roll(high, -2, 0)
            value = widen(c, e - 2, lk[at], low, high)
        elif e == 0:
            value = far_rows(xtwo[c % PAIRS], None, None, c // PAIRS)
        elif e == 1:
            low = pick(c_ll, c) if d == 0 else (pick(c_ll, MAT + c) if d == 3 else None)
            value = far_rows(xfar[0, (d // 2) * MAT + c], low, pick(c_lh, c) if d == 0 else None, d % 2)
        else:
            value = far_rows(xfar[1, (d // 2) * MAT + c], pick(c_hl, c) if d == 3 else None, None, d % 2)
        if d == 0:
            return 0.5 * value
        if d == 1:
            return (0.5 * sign) * value
        if d == 2:
            return (0.5 * sign) * y_sign * value
        return sign * yz_sign * edge * value

    def build(rows):
        for part_no in range(2):
            for i in range(3):
                for j in range(3):
                    c = part_no * PAIRS + i * 3 + j
                    flip = part_no * PAIRS + j * 3 + i
                    back = 1.0 if part_no else -1.0
                    for e in rows:
                        wx = wide_link(0, c, e)
                        if e > 0:
                            gauge[0, c, e - 1] = wx
                        if e < 4:
                            gauge[1, flip, e] = back * wx
                        if e == 0:
                            continue
                        wz = wide_link(2, c, e)
                        gauge[3, c, e - 1] = wz
                        gauge[4, flip, e - 1] = back * z_dn(wz)
                        wt = wide_link(3, c, e)
                        gauge[5, c, e - 1] = wt
                        gauge[6, flip, e - 1] = back * roll(wt, 1, 0)
                        wy = wide_link(1, c, e)
                        turned = wide_link(1, flip, e)
                        gauge[2, c, e - 1] = wy + back * roll(turned, NZ, 1)

    build((2, 3))
    for item in [copy(sx, xfar, lsend.at[1], lrecv.at[1], (g, zt, x_up))] + rest:
        item.wait()
    build((0, 1, 4))

    def finish_halo(par):
        copy(hb.at[par], hb.at[par], hsend.at[par], hrecv.at[par], corner_dev[0]).wait()

    wait_part(0)
    finish_halo(0)
    for c in range(COMPS):
        wide = extend(0, c)
        for e in range(6):
            dirn[c, e] = wide[e]
            resid[c, e] = wide[e]
    norm = fill(summed(lambda j: part[0, j]), 0)

    def hop(field, e0):
        total = [None] * COMPS
        terms = (
            (0, lambda c: field[c, e0 + 1:e0 + 3]),
            (1, lambda c: field[c, e0 - 1:e0 + 1]),
            (2, lambda c: roll(field[c, e0:e0 + 2], NZ, 2)),
            (3, lambda c: z_up(field[c, e0:e0 + 2])),
            (4, lambda c: z_dn(field[c, e0:e0 + 2])),
            (5, lambda c: roll(field[c, e0:e0 + 2], -1, 1)),
            (6, lambda c: roll(field[c, e0:e0 + 2], 1, 1)),
        )
        for term, shifted in terms:
            v = [shifted(c) for c in range(COMPS)]
            for i in range(3):
                for j in range(3):
                    wre = gauge[term, i * 3 + j, e0 - 1:e0 + 1]
                    wim = gauge[term, PAIRS + i * 3 + j, e0 - 1:e0 + 1]
                    re = wre * v[j] - wim * v[3 + j]
                    im = wre * v[3 + j] + wim * v[j]
                    total[i] = re if total[i] is None else total[i] + re
                    total[3 + i] = im if total[3 + i] is None else total[3 + i] + im
        return total

    def image_of():
        for e0 in (1, 3):
            for c, value in enumerate(hop(dirn, e0)):
                mid[c, e0:e0 + 2] = value
        image = hop(mid, 2)
        packed = []
        dpack = []
        for c in range(COMPS):
            d2, d3 = dirn[c, 2], dirn[c, 3]
            dp = jnp.where(first, roll(d2, -2, 0), roll(d3, 2, 0))
            wp = jnp.where(first, roll(image[c][0], -2, 0), roll(image[c][1], 2, 0))
            dpack.append(dp)
            packed.append(mass_sq * dp - wp)
        return packed, dpack

    def row(values, k):
        return jnp.broadcast_to(values[k:k + 1], (8, lanes))

    def accumulate(gain):
        for c in range(COMPS):
            total = out_ref[c]
            for k in range(nshift):
                total = total + row(gain, k) * shiftdirs[k, c]
            out_ref[c] = total

    def catch_up(gain, zeta_now, beta_shift):
        accumulate(gain)
        for k in range(nshift):
            zk, bk = row(zeta_now, k), row(beta_shift, k)
            for c in range(COMPS):
                shiftdirs[k, c] = zk * rpack[c] + bk * shiftdirs[k, c]

    lane16 = lax.broadcasted_iota(jnp.int32, (16, lanes), 1)
    swap = copy(mine, theirs, asend.at[1], arecv.at[1], (other, zt, xy))

    def closing(sums, values):
        norm, zeta, zeta_old, alpha_old, beta_old, beta_shift, along, score = values
        alpha = norm / fill(sums, 0)
        zeta_new = zeta * zeta_old * alpha_old / (
            alpha * beta_old * (zeta_old - zeta) + zeta_old * alpha_old * (1.0 + shift_rows * alpha)
        )
        gain = residue_rows * alpha * (zeta_new / zeta)
        return gain, score + gain * (zeta * fill(sums, 3) + beta_shift * along)

    def iterate(step, last):
        norm, zeta, zeta_old, alpha_old, beta_old, beta_shift, along, score, gain = [state[k] for k in range(9)]
        par = step % 2 if last else lax.rem(step, 2)
        if last:
            packed_state = norm
            for k in range(1, 8):
                packed_state = jnp.where(lane16 == k, state[k], packed_state)
            mine[...] = packed_state
            swap.start()
        packed, dpack = image_of()
        res = [rpack[c] for c in range(COMPS)]
        part[par, pl.ds(me, 1)] = dots([inner(dpack, packed), inner(res, packed), inner(packed, packed), inner(spack, res)])[None]
        send_part(par)
        if last:
            send_cross(par)
        else:
            corner_tiles(packed, par)
            for c in range(COMPS):
                ws[par, c] = packed[c]
            for item in halo(par):
                item.start()
        catch_up(gain, zeta, beta_shift)
        wait_part(par)
        sums = summed(lambda j: part[par, j])
        if last:
            gain, score = closing(sums, [state[k] for k in range(8)])
            accumulate(gain)
            return score
        alpha = norm / fill(sums, 0)
        zeta_new = zeta * zeta_old * alpha_old / (
            alpha * beta_old * (zeta_old - zeta) + zeta_old * alpha_old * (1.0 + shift_rows * alpha)
        )
        ratio = zeta_new / zeta
        along = zeta * fill(sums, 3) + beta_shift * along
        gain = residue_rows * alpha * ratio
        score = score + gain * along
        norm_next = norm - 2.0 * alpha * fill(sums, 1) + alpha * alpha * fill(sums, 2)
        beta = norm_next / norm
        beta_shift = beta * ratio * ratio
        finish_halo(par)
        step_a, step_b = row(alpha, 0), row(beta, 0)
        for c in range(COMPS):
            rpack[c] = rpack[c] - step_a * ws[par, c]
            wide = extend(par, c)
            for e in range(6):
                fresh = resid[c, e] - step_a * wide[e]
                resid[c, e] = fresh
                dirn[c, e] = fresh + step_b * dirn[c, e]
        for k, value in enumerate((norm_next, zeta_new, zeta, alpha, beta, beta_shift, along, score, gain)):
            state[k] = value

    one = jnp.ones((16, lanes), jnp.float32)
    none = jnp.zeros((16, lanes), jnp.float32)

    def body(step, carry):
        iterate(step, False)
        return carry

    for k, value in enumerate((norm, one, one, one, none, none, none, none, none)):
        state[k] = value
    lax.fori_loop(1, ITERS, body, 0)
    score = iterate(ITERS, True)
    swap.wait()
    copy(cross, cross, asend.at[0], arecv.at[0], corner_dev[0]).wait()
    far_state = theirs[...]
    values = [jnp.broadcast_to(far_state[:, k:k + 1], (16, lanes)) for k in range(8)]
    total = score + closing(summed(lambda j: cross[j]), values)[1]
    sites = n_grp * n_all * cells_x * cells_t * lanes
    action_ref[0] = jnp.max(jnp.sum(total, axis=0, keepdims=True)) * (1.0 / sites)


def on_device(sizes, source, links, shifts, residues, mass):
    n_grp, n_zt, n_xy = sizes
    cells_x, cells_t, lanes = source.shape[3:]
    n_all = n_zt * n_xy
    f32 = jnp.float32
    tiles = lambda *lead: pltpu.VMEM(lead + (8, lanes), f32)
    rows = lambda count: pltpu.VMEM((count, lanes), f32)
    nshift = shifts.shape[0]
    vmem = pl.BlockSpec(memory_space=pltpu.VMEM)
    smem = pl.BlockSpec(memory_space=pltpu.SMEM)
    dma = pltpu.SemaphoreType.DMA
    rational, action = pl.pallas_call(
        functools.partial(kernel, (n_grp, n_zt, n_xy, cells_x, cells_t)),
        out_shape=(
            pltpu.VMEM((COMPS, 8, lanes), f32),
            pltpu.SMEM((1,), f32),
        ),
        in_specs=[pl.BlockSpec(memory_space=pltpu.HBM)] * 5,
        out_specs=(vmem, smem),
        scratch_shapes=[
            tiles(4 * MAT), tiles(2, 2 * MAT), tiles(2, 2 * MAT), tiles(PAIRS), tiles(2, 2 * MAT), tiles(2, 2 * MAT), tiles(PAIRS),
            rows(40), rows(24), rows(24), rows(40), rows(24), rows(24),
            tiles(7, MAT, 4), tiles(COMPS, 6), tiles(COMPS, 6), tiles(COMPS, 6),
            tiles(nshift, COMPS), tiles(COMPS), tiles(2, COMPS), tiles(2, 4), tiles(2, 4 * COMPS + 4),
            pltpu.VMEM((2, n_all, 1, lanes), f32), pltpu.VMEM((n_all, 1, lanes), f32),
            pltpu.VMEM((9, 16, lanes), f32), rows(16), rows(16), tiles(COMPS), tiles(2 * MAT),
            pltpu.SMEM((nshift,), f32), pltpu.SMEM((nshift,), f32), pltpu.SMEM((1,), f32), dma((5,)),
            dma((7,)), dma((7,)), dma((2,)), dma((2,)), dma((2,)), dma((2,)), dma((2,)), dma((2,)),
        ],
        compiler_params=pltpu.CompilerParams(collective_id=0, has_side_effects=True),
    )(
        source.reshape(COMPS, 8, lanes), links.reshape(2 * MAT, 8, lanes), shifts, residues, mass
    )
    return rational.reshape(source.shape), action


def solution(mesh):
    sizes = tuple(mesh.shape[name] for name in ("grp", "zt", "xy"))
    field = P("grp", None, None, "xy", "zt", None)
    return jax.shard_map(
        functools.partial(on_device, sizes),
        mesh=mesh,
        in_specs=(field, P("grp", None, None, None, "xy", "zt", None), P(), P(), P()),
        out_specs=(field, P()),
        check_vma=False,
    )
```

```python
import functools

import jax
import jax.numpy as jnp
from jax import lax
from jax.experimental import pallas as pl
from jax.experimental.pallas import tpu as pltpu
from jax.sharding import PartitionSpec as P

NY = 2
NZ = 64
ITERS = 8
PAIRS = 9
MAT = 2 * PAIRS
COMPS = 6


def roll(value, shift, axis):
    size = value.shape[axis]
    return pltpu.roll(value, shift % size, axis)


def kernel(
    dims, source_hbm, links_hbm, shifts_hbm, residues_hbm, mass_hbm, out_ref, action_ref,
    lk, tfar, xfar, xtwo, sx, st, sx2, cs_ll, cs_hl, cs_lh, c_ll, c_hl, c_lh,
    gauge, wide, hop_w, hop_r, mid, dpack_ref, shiftdirs, rpack, ws, cs, hb, part, cross,
    state, mine, theirs, source_ref, links_ref, shifts_ref, residues_ref, mass_ref,
    isem, lsend, lrecv, hsend, hrecv, psend, precv, asend, arecv,
):
    n_grp, n_zt, n_xy, cells_x, cells_t = dims
    lanes = NY * NZ
    n_all = n_zt * n_xy
    nshift = shifts_ref.shape[0]
    g = lax.axis_index("grp")
    zt = lax.axis_index("zt")
    xy = lax.axis_index("xy")
    me = zt * n_xy + xy
    me_all = g * n_all + me
    x_up, x_dn = lax.rem(xy + 1, n_xy), lax.rem(xy + n_xy - 1, n_xy)
    t_up, t_dn = lax.rem(zt + 1, n_zt), lax.rem(zt + n_zt - 1, n_zt)
    other = 1 - g

    def place(linear):
        inside = lax.rem(linear, n_all)
        return (linear // n_all, inside // n_xy, lax.rem(inside, n_xy))

    def each(count, fn):
        if count <= 32:
            for p in range(1, count):
                fn(p)
        else:
            def step(p, carry):
                fn(p)
                return carry
            lax.fori_loop(1, count, step, 0)

    def copy(src, dst, send, recv, device):
        return pltpu.make_async_remote_copy(
            src_ref=src, dst_ref=dst, send_sem=send, recv_sem=recv,
            device_id=device, device_id_type=pl.DeviceIdType.MESH,
        )

    barrier = pltpu.get_barrier_semaphore()

    corner_dev = ((g, t_up, x_up), (g, t_dn, x_up), (g, t_up, x_dn), (g, t_dn, x_dn))
    partners = ((other, zt, xy), (g, zt, x_up), (g, zt, x_dn), (g, t_up, xy), (g, t_dn, xy)) + corner_dev
    near_barrier = n_zt <= 4 and n_xy <= 4

    def greet(device):
        pl.semaphore_signal(barrier, inc=1, device_id=device, device_id_type=pl.DeviceIdType.MESH)

    fetch_links = pltpu.make_async_copy(links_hbm, links_ref, isem.at[0])
    fetch_source = pltpu.make_async_copy(source_hbm, source_ref, isem.at[1])
    if near_barrier:
        for device in partners:
            greet(device)
    else:
        each(n_grp * n_all, lambda p: greet(place(lax.rem(me_all + p, n_grp * n_all))))
    fetch_links.start()
    fetch_source.start()
    scalars = [
        pltpu.make_async_copy(src, dst, isem.at[2 + k])
        for k, (src, dst) in enumerate(((shifts_hbm, shifts_ref), (residues_hbm, residues_ref), (mass_hbm, mass_ref)))
    ]
    for item in scalars:
        item.start()
    fetch_links.wait()
    fetch_source.wait()

    sub = lax.broadcasted_iota(jnp.int32, (8, lanes), 0)
    lane = lax.broadcasted_iota(jnp.int32, (8, lanes), 1)
    zcoord = lax.rem(lane, NZ)
    ycoord = lane // NZ
    quarter = lanes // 4
    home = sub == lane // quarter
    own = (sub >= 2) & (sub < 2 + cells_t)
    first = sub < cells_t
    late = lax.rem(sub, cells_t) >= 2

    def t_faces(c, one, two):
        st[0, pl.ds(c, 1)] = jnp.where(late, one, roll(two, -2, 0))[None]
        st[1, pl.ds(c, 1)] = jnp.where(late, roll(two, 2, 0), one)[None]

    for d in range(2):
        for c in range(MAT):
            low, high = links_ref[c], links_ref[MAT + c]
            if d == 0:
                sx[0, pl.ds(g * MAT + c, 1)] = jnp.where(first, roll(low, 4, 0), high)[None]
            else:
                sx[1, pl.ds(g * MAT + c, 1)] = jnp.where(first, low, roll(high, 4, 0))[None]
    for c in range(MAT):
        t_faces(g * MAT + c, links_ref[c], links_ref[MAT + c])
    for c in range(2 * MAT):
        lk[pl.ds(g * 2 * MAT + c, 1)] = links_ref[c][None]

    spack = [source_ref[c] for c in range(COMPS)]

    def corner_tiles(tiles, par):
        for k, row in enumerate((7, 4, 3, 0)):
            tile = jnp.zeros((8, lanes), jnp.float32)
            for c in range(COMPS):
                tile = jnp.where(sub == c, jnp.broadcast_to(tiles[c][row:row + 1], (8, lanes)), tile)
            cs[par, k] = tile

    def halo(par):
        k_first = jnp.where(xy == 0, 1, 0)
        routes = (
            (k_first, (g, zt, jnp.where(xy == 0, x_dn, x_up))), (1 - k_first, (g, zt, jnp.where(xy == 0, x_up, x_dn))),
            (2, (g, t_up, xy)), (3, (g, t_dn, xy)),
        )
        found = []
        for k in range(4):
            found.append(copy(cs.at[par, pl.ds(k, 1)], hb.at[par, pl.ds(4 * COMPS + k, 1)], hsend.at[par], hrecv.at[par], corner_dev[k]))
        for k, device in routes:
            found.append(copy(ws.at[par], hb.at[par, pl.ds(k * COMPS, COMPS)], hsend.at[par], hrecv.at[par], device))
        return found

    def send_part(par):
        def go(p):
            copy(part.at[par, me], part.at[par, me], psend.at[par], precv.at[par],
                 (g,) + place(lax.rem(me + p, n_all))[1:]).start()
        each(n_all, go)

    def wait_part(par):
        rest = part.at[par, pl.ds(0, n_all - 1)]
        copy(rest, rest, psend.at[par], precv.at[par], corner_dev[0]).wait()

    def send_cross(par):
        def go(p):
            copy(part.at[par, me], cross.at[me], asend.at[0], arecv.at[0],
                 (other,) + place(lax.rem(me + p, n_all))[1:]).start()
        go(0)
        each(n_all, go)

    def dots(rows):
        tile = jnp.zeros((8, lanes), jnp.float32)
        for k, row in enumerate(rows):
            tile = jnp.where(sub == k, jnp.broadcast_to(jnp.sum(row, axis=0, keepdims=True), (8, lanes)), tile)
        tile = (tile + roll(tile, 2 * quarter, 1)) + (roll(tile, quarter, 1) + roll(tile, 3 * quarter, 1))
        return jnp.sum(jnp.where(home, tile, 0.0), axis=0, keepdims=True)

    def summed(row_of):
        if n_all <= 32:
            level = [row_of(j) for j in range(n_all)]
            while len(level) > 1:
                odd = level[len(level) // 2 * 2:]
                level = [level[k] + level[k + 1] for k in range(0, len(level) - 1, 2)] + odd
            total = level[0]
        else:
            total = lax.fori_loop(1, n_all, lambda j, acc: acc + row_of(j), row_of(0))
        split = jnp.where(home, jnp.broadcast_to(total, (8, lanes)), 0.0)
        return jnp.broadcast_to(jnp.sum(split, axis=1, keepdims=True), (8, lanes))

    def fill(values, k):
        return jnp.broadcast_to(values[k:k + 1], (16, lanes))

    def inner(left, right):
        total = left[0] * right[0]
        for c in range(1, COMPS):
            total = total + left[c] * right[c]
        return total

    corner_tiles(spack, 0)
    for c in range(COMPS):
        ws[0, c] = spack[c]

    pl.semaphore_wait(barrier, len(partners) if near_barrier else n_grp * n_all - 1)

    half = 2 * MAT
    to_pair = copy(links_ref, lk.at[pl.ds(g * half, half)], lsend.at[0], lrecv.at[0], (other, zt, xy))
    to_pair.start()

    def link_faces(h):
        span = pl.ds(h * MAT, MAT)
        return [
            copy(sx.at[0, span], xfar.at[0, span], lsend.at[1], lrecv.at[1], (g, zt, x_up)),
            copy(sx.at[1, span], xfar.at[1, span], lsend.at[1], lrecv.at[1], (g, zt, x_dn)),
            copy(st.at[0, span], tfar.at[0, span], lsend.at[2], lrecv.at[2], (g, t_up, xy)),
            copy(st.at[1, span], tfar.at[1, span], lsend.at[2], lrecv.at[2], (g, t_dn, xy)),
        ]

    for item in link_faces(g):
        item.start()
    for item in halo(0):
        item.start()

    to_pair.wait_recv()
    for c in range(MAT):
        low, high = lk[other * half + c], lk[other * half + MAT + c]
        sx[0, pl.ds(other * MAT + c, 1)] = jnp.where(first, roll(low, 4, 0), high)[None]
        sx[1, pl.ds(other * MAT + c, 1)] = jnp.where(first, low, roll(high, 4, 0))[None]
        t_faces(other * MAT + c, low, high)
    for c in range(PAIRS):
        sx2[c] = jnp.where(first, lk[c], roll(lk[PAIRS + c], 4, 0))
    for c in range(MAT):
        cs_ll[c:c + 1] = lk[c][7:8]
        cs_ll[MAT + c:MAT + c + 1] = lk[3 * MAT + c][7:8]
        cs_hl[c:c + 1] = lk[3 * MAT + c][3:4]
        cs_lh[c:c + 1] = lk[c][4:5]
    rest = [
        copy(sx2, xtwo, lsend.at[3], lrecv.at[3], (g, zt, x_up)),
        copy(cs_ll, c_ll, lsend.at[4], lrecv.at[4], corner_dev[0]),
        copy(cs_hl, c_hl, lsend.at[5], lrecv.at[5], corner_dev[2]),
        copy(cs_lh, c_lh, lsend.at[6], lrecv.at[6], corner_dev[1]),
    ]
    for item in rest + link_faces(other):
        item.start()

    def pick(ref, c):
        return jnp.broadcast_to(ref[c:c + 1], (8, lanes))

    def widen(c, x, mine, low, high):
        between = jnp.where(late, low, high)
        return jnp.where(own, roll(mine, 2 - 4 * x, 0), roll(between, 6 - 4 * x, 0))

    def far_rows(block, low_corner, high_corner, x):
        row = jnp.where(own, roll(block, 2 - 4 * x, 0), 0.0)
        if low_corner is not None:
            row = jnp.where(sub == 1, low_corner, row)
        if high_corner is not None:
            row = jnp.where(sub == 6, high_corner, row)
        return row

    def extend(par, c):
        own_part = ws[par, c]
        corner = [jnp.broadcast_to(hb[par, 4 * COMPS + k, c:c + 1], (8, lanes)) for k in range(4)]
        x_lo, x_hi, t_lo, t_hi = [hb[par, k * COMPS + c] for k in range(4)]
        return [
            far_rows(x_lo, None, None, 0),
            far_rows(x_lo, corner[0], corner[1], 1),
            widen(c, 0, own_part, t_lo, t_hi),
            widen(c, 1, own_part, t_lo, t_hi),
            far_rows(x_hi, corner[2], corner[3], 0),
            far_rows(x_hi, None, None, 1),
        ]

    for item in scalars:
        item.wait()
    rows16 = lax.broadcasted_iota(jnp.int32, (16, lanes), 0)
    shift_rows = jnp.zeros((16, lanes), jnp.float32)
    residue_rows = jnp.zeros((16, lanes), jnp.float32)
    for k in range(nshift):
        shift_rows = jnp.where(rows16 == k, shifts_ref[k], shift_rows)
        residue_rows = jnp.where(rows16 == k, residues_ref[k], residue_rows)
    mass_sq = mass_ref[0] * mass_ref[0]

    for c in range(COMPS):
        rpack[c] = spack[c]
        out_ref[c] = jnp.zeros((8, lanes), jnp.float32)
        for k in range(nshift):
            shiftdirs[k, c] = spack[c]

    copy(st, tfar, lsend.at[2], lrecv.at[2], (g, t_up, xy)).wait()
    to_pair.wait_send()

    t_at = lax.rem(zt * cells_t + sub - 2 + n_zt * cells_t, n_zt * cells_t)
    edge = jnp.where(t_at == n_zt * cells_t - 1, -0.5, 0.5)
    yz_sign = (1 - 2 * lax.rem(ycoord + zcoord, 2)).astype(jnp.float32)
    y_sign = (1 - 2 * lax.rem(ycoord, 2)).astype(jnp.float32)

    def z_up(v):
        cond = jnp.broadcast_to(zcoord == NZ - 1, v.shape)
        return jnp.where(cond, roll(v, NZ - 1, v.ndim - 1), roll(v, -1, v.ndim - 1))

    def z_dn(v):
        cond = jnp.broadcast_to(zcoord == 0, v.shape)
        return jnp.where(cond, roll(v, 1 - NZ, v.ndim - 1), roll(v, 1, v.ndim - 1))

    def wide_link(d, c, e):
        at = d * MAT + c
        sign = -1.0 if e % 2 else 1.0
        if e in (2, 3):
            low, high = tfar[0, (d // 2) * MAT + c], tfar[1, (d // 2) * MAT + c]
            if d % 2:
                low, high = roll(low, 2, 0), roll(high, -2, 0)
            value = widen(c, e - 2, lk[at], low, high)
        elif e == 0:
            value = far_rows(xtwo[c % PAIRS], None, None, c // PAIRS)
        elif e == 1:
            low = pick(c_ll, c) if d == 0 else (pick(c_ll, MAT + c) if d == 3 else None)
            value = far_rows(xfar[0, (d // 2) * MAT + c], low, pick(c_lh, c) if d == 0 else None, d % 2)
        else:
            value = far_rows(xfar[1, (d // 2) * MAT + c], pick(c_hl, c) if d == 3 else None, None, d % 2)
        if d == 0:
            return 0.5 * value
        if d == 1:
            return (0.5 * sign) * value
        if d == 2:
            return (0.5 * sign) * y_sign * value
        return sign * yz_sign * edge * value

    def build(rows):
        for part_no in range(2):
            for i in range(3):
                for j in range(3):
                    c = part_no * PAIRS + i * 3 + j
                    flip = part_no * PAIRS + j * 3 + i
                    back = 1.0 if part_no else -1.0
                    for e in rows:
                        wx = wide_link(0, c, e)
                        if e > 0:
                            gauge[0, c, e - 1] = wx
                        if e < 4:
                            gauge[1, flip, e] = back * wx
                        if e == 0:
                            continue
                        wz = wide_link(2, c, e)
                        gauge[3, c, e - 1] = wz
                        gauge[4, flip, e - 1] = back * z_dn(wz)
                        wt = wide_link(3, c, e)
                        gauge[5, c, e - 1] = wt
                        gauge[6, flip, e - 1] = back * roll(wt, 1, 0)
                        wy = wide_link(1, c, e)
                        turned = wide_link(1, flip, e)
                        gauge[2, c, e - 1] = wy + back * roll(turned, NZ, 1)

    build((2, 3))
    for item in [copy(sx, xfar, lsend.at[1], lrecv.at[1], (g, zt, x_up))] + rest:
        item.wait()
    build((0, 1, 4))

    def finish_halo(par):
        copy(hb.at[par], hb.at[par], hsend.at[par], hrecv.at[par], corner_dev[0]).wait()

    finish_halo(0)

    def hop(field, e0):
        total = [None] * COMPS
        terms = (
            (0, lambda c: field[c, e0 + 1:e0 + 3]),
            (1, lambda c: field[c, e0 - 1:e0 + 1]),
            (2, lambda c: roll(field[c, e0:e0 + 2], NZ, 2)),
            (3, lambda c: z_up(field[c, e0:e0 + 2])),
            (4, lambda c: z_dn(field[c, e0:e0 + 2])),
            (5, lambda c: roll(field[c, e0:e0 + 2], -1, 1)),
            (6, lambda c: roll(field[c, e0:e0 + 2], 1, 1)),
        )
        for term, shifted in terms:
            v = [shifted(c) for c in range(COMPS)]
            for i in range(3):
                for j in range(3):
                    wre = gauge[term, i * 3 + j, e0 - 1:e0 + 1]
                    wim = gauge[term, PAIRS + i * 3 + j, e0 - 1:e0 + 1]
                    re = wre * v[j] - wim * v[3 + j]
                    im = wre * v[3 + j] + wim * v[j]
                    total[i] = re if total[i] is None else total[i] + re
                    total[3 + i] = im if total[3 + i] is None else total[3 + i] + im
        return total

    def hop_wide(par):
        for c in range(COMPS):
            for e, value in enumerate(extend(par, c)):
                wide[c, e] = value
        for e0 in (1, 3):
            for c, value in enumerate(hop(wide, e0)):
                hop_w[c, e0:e0 + 2] = value

    hop_wide(0)
    for c in range(COMPS):
        dpack_ref[c] = spack[c]
        hop_r[c, 1:5] = hop_w[c, 1:5]
        mid[c, 1:5] = hop_w[c, 1:5]

    def image_of():
        image = hop(mid, 2)
        packed = []
        for c in range(COMPS):
            wp = jnp.where(first, roll(image[c][0], -2, 0), roll(image[c][1], 2, 0))
            packed.append(mass_sq * dpack_ref[c] - wp)
        return packed, [dpack_ref[c] for c in range(COMPS)]

    def row(values, k):
        return jnp.broadcast_to(values[k:k + 1], (8, lanes))

    def accumulate(gain):
        for c in range(COMPS):
            total = out_ref[c]
            for k in range(nshift):
                total = total + row(gain, k) * shiftdirs[k, c]
            out_ref[c] = total

    def catch_up(gain, zeta_now, beta_shift):
        accumulate(gain)
        for k in range(nshift):
            zk, bk = row(zeta_now, k), row(beta_shift, k)
            for c in range(COMPS):
                shiftdirs[k, c] = zk * rpack[c] + bk * shiftdirs[k, c]

    lane16 = lax.broadcasted_iota(jnp.int32, (16, lanes), 1)
    swap = copy(mine, theirs, asend.at[1], arecv.at[1], (other, zt, xy))

    def closing(sums, values):
        norm, zeta, zeta_old, alpha_old, beta_old, beta_shift, along, score = values
        alpha = norm / fill(sums, 0)
        zeta_new = zeta * zeta_old * alpha_old / (
            alpha * beta_old * (zeta_old - zeta) + zeta_old * alpha_old * (1.0 + shift_rows * alpha)
        )
        gain = residue_rows * alpha * (zeta_new / zeta)
        return gain, score + gain * (zeta * fill(sums, 3) + beta_shift * along)

    def iterate(step, last):
        norm, zeta, zeta_old, alpha_old, beta_old, beta_shift, along, score, gain = [state[k] for k in range(9)]
        par = step % 2 if last else lax.rem(step, 2)
        if last:
            packed_state = norm
            for k in range(1, 8):
                packed_state = jnp.where(lane16 == k, state[k], packed_state)
            mine[...] = packed_state
            swap.start()
        packed, dpack = image_of()
        res = [rpack[c] for c in range(COMPS)]
        part[par, pl.ds(me, 1)] = dots([inner(dpack, packed), inner(res, packed), inner(packed, packed), inner(spack, res)])[None]
        send_part(par)
        if last:
            send_cross(par)
        else:
            corner_tiles(packed, par)
            for c in range(COMPS):
                ws[par, c] = packed[c]
            for item in halo(par):
                item.start()
        catch_up(gain, zeta, beta_shift)
        if not last:
            finish_halo(par)
            hop_wide(par)
        wait_part(par)
        sums = summed(lambda j: part[par, j])
        if last:
            gain, score = closing(sums, [state[k] for k in range(8)])
            accumulate(gain)
            return score
        norm = jnp.where(step == 1, fill(sums, 3), norm)
        alpha = norm / fill(sums, 0)
        zeta_new = zeta * zeta_old * alpha_old / (
            alpha * beta_old * (zeta_old - zeta) + zeta_old * alpha_old * (1.0 + shift_rows * alpha)
        )
        ratio = zeta_new / zeta
        along = zeta * fill(sums, 3) + beta_shift * along
        gain = residue_rows * alpha * ratio
        score = score + gain * along
        norm_next = norm - 2.0 * alpha * fill(sums, 1) + alpha * alpha * fill(sums, 2)
        beta = norm_next / norm
        beta_shift = beta * ratio * ratio
        step_a, step_b = row(alpha, 0), row(beta, 0)
        for c in range(COMPS):
            fresh = rpack[c] - step_a * ws[par, c]
            rpack[c] = fresh
            dpack_ref[c] = fresh + step_b * dpack_ref[c]
            for e in range(1, 5):
                fresh = hop_r[c, e] - step_a * hop_w[c, e]
                hop_r[c, e] = fresh
                mid[c, e] = fresh + step_b * mid[c, e]
        for k, value in enumerate((norm_next, zeta_new, zeta, alpha, beta, beta_shift, along, score, gain)):
            state[k] = value

    one = jnp.ones((16, lanes), jnp.float32)
    none = jnp.zeros((16, lanes), jnp.float32)

    def body(step, carry):
        iterate(step, False)
        return carry

    for k, value in enumerate((one, one, one, one, none, none, none, none, none)):
        state[k] = value
    lax.fori_loop(1, ITERS, body, 0)
    score = iterate(ITERS, True)
    swap.wait()
    copy(cross, cross, asend.at[0], arecv.at[0], corner_dev[0]).wait()
    far_state = theirs[...]
    values = [jnp.broadcast_to(far_state[:, k:k + 1], (16, lanes)) for k in range(8)]
    total = score + closing(summed(lambda j: cross[j]), values)[1]
    sites = n_grp * n_all * cells_x * cells_t * lanes
    action_ref[0] = jnp.max(jnp.sum(total, axis=0, keepdims=True)) * (1.0 / sites)


def on_device(sizes, source, links, shifts, residues, mass):
    n_grp, n_zt, n_xy = sizes
    cells_x, cells_t, lanes = source.shape[3:]
    n_all = n_zt * n_xy
    f32 = jnp.float32
    tiles = lambda *lead: pltpu.VMEM(lead + (8, lanes), f32)
    rows = lambda count: pltpu.VMEM((count, lanes), f32)
    nshift = shifts.shape[0]
    vmem = pl.BlockSpec(memory_space=pltpu.VMEM)
    smem = pl.BlockSpec(memory_space=pltpu.SMEM)
    dma = pltpu.SemaphoreType.DMA
    rational, action = pl.pallas_call(
        functools.partial(kernel, (n_grp, n_zt, n_xy, cells_x, cells_t)),
        out_shape=(
            pltpu.VMEM((COMPS, 8, lanes), f32),
            pltpu.SMEM((1,), f32),
        ),
        in_specs=[pl.BlockSpec(memory_space=pltpu.HBM)] * 5,
        out_specs=(vmem, smem),
        scratch_shapes=[
            tiles(4 * MAT), tiles(2, 2 * MAT), tiles(2, 2 * MAT), tiles(PAIRS), tiles(2, 2 * MAT), tiles(2, 2 * MAT), tiles(PAIRS),
            rows(40), rows(24), rows(24), rows(40), rows(24), rows(24),
            tiles(7, MAT, 4), tiles(COMPS, 6), tiles(COMPS, 6), tiles(COMPS, 6), tiles(COMPS, 6), tiles(COMPS),
            tiles(nshift, COMPS), tiles(COMPS), tiles(2, COMPS), tiles(2, 4), tiles(2, 4 * COMPS + 4),
            pltpu.VMEM((2, n_all, 1, lanes), f32), pltpu.VMEM((n_all, 1, lanes), f32),
            pltpu.VMEM((9, 16, lanes), f32), rows(16), rows(16), tiles(COMPS), tiles(2 * MAT),
            pltpu.SMEM((nshift,), f32), pltpu.SMEM((nshift,), f32), pltpu.SMEM((1,), f32), dma((5,)),
            dma((7,)), dma((7,)), dma((2,)), dma((2,)), dma((2,)), dma((2,)), dma((2,)), dma((2,)),
        ],
        compiler_params=pltpu.CompilerParams(collective_id=0, has_side_effects=True),
    )(
        source.reshape(COMPS, 8, lanes), links.reshape(2 * MAT, 8, lanes), shifts, residues, mass
    )
    return rational.reshape(source.shape), action


def solution(mesh):
    sizes = tuple(mesh.shape[name] for name in ("grp", "zt", "xy"))
    field = P("grp", None, None, "xy", "zt", None)
    return jax.shard_map(
        functools.partial(on_device, sizes),
        mesh=mesh,
        in_specs=(field, P("grp", None, None, None, "xy", "zt", None), P(), P(), P()),
        out_specs=(field, P()),
        check_vma=False,
    )
```

```python
import functools

import jax
import jax.numpy as jnp
from jax import lax
from jax.experimental import pallas as pl
from jax.experimental.pallas import tpu as pltpu
from jax.sharding import PartitionSpec as P

NY = 2
NZ = 64
ITERS = 8
PAIRS = 9
MAT = 2 * PAIRS
COMPS = 6


def roll(value, shift, axis):
    size = value.shape[axis]
    return pltpu.roll(value, shift % size, axis)


def kernel(
    dims, source_hbm, links_hbm, shifts_hbm, residues_hbm, mass_hbm, out_ref, action_ref,
    lk, tfar, xfar, xtwo, sx, st, sx2, cs_ll, cs_hl, cs_lh, c_ll, c_hl, c_lh,
    gauge, wide, hop_w, hop_r, mid, dpack_ref, shiftdirs, rpack, ws, cs, hb, part, cross,
    state, mine, theirs, source_ref, links_ref, shifts_ref, residues_ref, mass_ref,
    isem, lsend, lrecv, hsend, hrecv, psend, precv, asend, arecv, ready,
):
    n_grp, n_zt, n_xy, cells_x, cells_t = dims
    lanes = NY * NZ
    n_all = n_zt * n_xy
    nshift = shifts_ref.shape[0]
    g = lax.axis_index("grp")
    zt = lax.axis_index("zt")
    xy = lax.axis_index("xy")
    me = zt * n_xy + xy
    me_all = g * n_all + me
    x_up, x_dn = lax.rem(xy + 1, n_xy), lax.rem(xy + n_xy - 1, n_xy)
    t_up, t_dn = lax.rem(zt + 1, n_zt), lax.rem(zt + n_zt - 1, n_zt)
    other = 1 - g

    def place(linear):
        inside = lax.rem(linear, n_all)
        return (linear // n_all, inside // n_xy, lax.rem(inside, n_xy))

    def each(count, fn):
        if count <= 32:
            for p in range(1, count):
                fn(p)
        else:
            def step(p, carry):
                fn(p)
                return carry
            lax.fori_loop(1, count, step, 0)

    def copy(src, dst, send, recv, device):
        return pltpu.make_async_remote_copy(
            src_ref=src, dst_ref=dst, send_sem=send, recv_sem=recv,
            device_id=device, device_id_type=pl.DeviceIdType.MESH,
        )

    barrier = pltpu.get_barrier_semaphore()

    corner_dev = ((g, t_up, x_up), (g, t_dn, x_up), (g, t_up, x_dn), (g, t_dn, x_dn))
    above = ((g, zt, x_up),) + corner_dev[:2]
    partners = ((other, zt, xy), (g, t_up, xy), (g, t_dn, xy), (g, zt, x_dn)) + corner_dev[2:]
    near_barrier = n_zt <= 4 and n_xy <= 4
    at_top, at_bottom = xy == n_xy - 1, xy == 0

    def greet(device):
        pl.semaphore_signal(barrier, inc=1, device_id=device, device_id_type=pl.DeviceIdType.MESH)

    fetch_links = pltpu.make_async_copy(links_hbm, links_ref, isem.at[0])
    fetch_source = pltpu.make_async_copy(source_hbm, source_ref, isem.at[1])
    if near_barrier:
        for device in partners:
            greet(device)

        @pl.when(jnp.logical_not(at_top))
        def _():
            for device in above:
                greet(device)
    else:
        each(n_grp * n_all, lambda p: greet(place(lax.rem(me_all + p, n_grp * n_all))))
    fetch_links.start()
    fetch_source.start()
    scalars = [
        pltpu.make_async_copy(src, dst, isem.at[2 + k])
        for k, (src, dst) in enumerate(((shifts_hbm, shifts_ref), (residues_hbm, residues_ref), (mass_hbm, mass_ref)))
    ]
    for item in scalars:
        item.start()
    fetch_links.wait()
    fetch_source.wait()

    sub = lax.broadcasted_iota(jnp.int32, (8, lanes), 0)
    lane = lax.broadcasted_iota(jnp.int32, (8, lanes), 1)
    zcoord = lax.rem(lane, NZ)
    ycoord = lane // NZ
    quarter = lanes // 4
    home = sub == lane // quarter
    own = (sub >= 2) & (sub < 2 + cells_t)
    first = sub < cells_t
    late = lax.rem(sub, cells_t) >= 2

    def t_faces(c, one, two):
        st[0, pl.ds(c, 1)] = jnp.where(late, one, roll(two, -2, 0))[None]
        st[1, pl.ds(c, 1)] = jnp.where(late, roll(two, 2, 0), one)[None]

    for d in range(2):
        for c in range(MAT):
            low, high = links_ref[c], links_ref[MAT + c]
            if d == 0:
                sx[0, pl.ds(g * MAT + c, 1)] = jnp.where(first, roll(low, 4, 0), high)[None]
            else:
                sx[1, pl.ds(g * MAT + c, 1)] = jnp.where(first, low, roll(high, 4, 0))[None]
    for c in range(MAT):
        t_faces(g * MAT + c, links_ref[c], links_ref[MAT + c])
    for c in range(2 * MAT):
        lk[pl.ds(g * 2 * MAT + c, 1)] = links_ref[c][None]

    spack = [source_ref[c] for c in range(COMPS)]

    def corner_tiles(tiles, par):
        for k, row in enumerate((7, 4, 3, 0)):
            tile = jnp.zeros((8, lanes), jnp.float32)
            for c in range(COMPS):
                tile = jnp.where(sub == c, jnp.broadcast_to(tiles[c][row:row + 1], (8, lanes)), tile)
            cs[par, k] = tile

    def face(par, k):
        device = ((g, zt, x_up), (g, zt, x_dn), (g, t_up, xy), (g, t_dn, xy))[k]
        return copy(ws.at[par], hb.at[par, pl.ds(k * COMPS, COMPS)], hsend.at[par], hrecv.at[par], device)

    def corner(par, k):
        return copy(cs.at[par, pl.ds(k, 1)], hb.at[par, pl.ds(4 * COMPS + k, 1)], hsend.at[par], hrecv.at[par], corner_dev[k])

    def start_halo(par):
        for k in range(4):
            corner(par, k).start()

        @pl.when(at_bottom)
        def _():
            face(par, 1).start()
        face(par, 0).start()

        @pl.when(jnp.logical_not(at_bottom))
        def _():
            face(par, 1).start()
        face(par, 2).start()
        face(par, 3).start()

    def send_part(par):
        def go(p):
            copy(part.at[par, me], part.at[par, me], psend.at[par], precv.at[par],
                 (g,) + place(lax.rem(me + p, n_all))[1:]).start()
        each(n_all, go)

    def wait_part(par):
        rest = part.at[par, pl.ds(0, n_all - 1)]
        copy(rest, rest, psend.at[par], precv.at[par], corner_dev[0]).wait()

    def send_cross(par):
        def go(p):
            copy(part.at[par, me], cross.at[me], asend.at[0], arecv.at[0],
                 (other,) + place(lax.rem(me + p, n_all))[1:]).start()
        go(0)
        each(n_all, go)

    def dots(rows):
        tile = jnp.zeros((8, lanes), jnp.float32)
        for k, row in enumerate(rows):
            tile = jnp.where(sub == k, jnp.broadcast_to(jnp.sum(row, axis=0, keepdims=True), (8, lanes)), tile)
        tile = (tile + roll(tile, 2 * quarter, 1)) + (roll(tile, quarter, 1) + roll(tile, 3 * quarter, 1))
        return jnp.sum(jnp.where(home, tile, 0.0), axis=0, keepdims=True)

    def summed(row_of):
        if n_all <= 32:
            level = [row_of(j) for j in range(n_all)]
            while len(level) > 1:
                odd = level[len(level) // 2 * 2:]
                level = [level[k] + level[k + 1] for k in range(0, len(level) - 1, 2)] + odd
            total = level[0]
        else:
            total = lax.fori_loop(1, n_all, lambda j, acc: acc + row_of(j), row_of(0))
        split = jnp.where(home, jnp.broadcast_to(total, (8, lanes)), 0.0)
        return jnp.broadcast_to(jnp.sum(split, axis=1, keepdims=True), (8, lanes))

    def fill(values, k):
        return jnp.broadcast_to(values[k:k + 1], (16, lanes))

    def inner(left, right):
        total = left[0] * right[0]
        for c in range(1, COMPS):
            total = total + left[c] * right[c]
        return total

    corner_tiles(spack, 0)
    for c in range(COMPS):
        ws[0, c] = spack[c]

    if near_barrier:
        pl.semaphore_wait(barrier, len(partners) + jnp.where(at_bottom, 0, len(above)))

        @pl.when(at_top)
        def _():
            for device in above:
                pl.semaphore_signal(ready, inc=1, device_id=device, device_id_type=pl.DeviceIdType.MESH)
    else:
        pl.semaphore_wait(barrier, n_grp * n_all - 1)

    half = 2 * MAT

    def to_pair(k):
        found = []
        for d in range(2):
            span = d * MAT + k * PAIRS
            found.append(copy(
                links_ref.at[pl.ds(span, PAIRS)], lk.at[pl.ds(g * half + span, PAIRS)],
                lsend.at[k], lrecv.at[k], (other, zt, xy),
            ))
        return found

    def span_of(h, k):
        return pl.ds(h * MAT + k * PAIRS, PAIRS)

    def up_face(h, k):
        span = span_of(h, k)
        return copy(sx.at[0, span], xfar.at[0, span], lsend.at[2], lrecv.at[2], (g, zt, x_up))

    def down_face(h, k):
        span = span_of(h, k)
        return copy(sx.at[1, span], xfar.at[1, span], lsend.at[2], lrecv.at[2], (g, zt, x_dn))

    def t_copies(h, k):
        span = span_of(h, k)
        return [
            copy(st.at[0, span], tfar.at[0, span], lsend.at[3], lrecv.at[3], (g, t_up, xy)),
            copy(st.at[1, span], tfar.at[1, span], lsend.at[3], lrecv.at[3], (g, t_dn, xy)),
        ]

    def below_near():
        for k in range(2):
            down_face(g, k).start()
        for k in (2, 3):
            corner(0, k).start()
        face(0, 1).start()

    for k in range(2):
        for item in to_pair(k):
            item.start()
    for k in range(2):
        for item in [up_face(g, k)] + t_copies(g, k):
            item.start()
    for k in (0, 1):
        corner(0, k).start()
    for k in (0, 2, 3):
        face(0, k).start()

    @pl.when(jnp.logical_not(at_bottom))
    def _():
        below_near()

    def pair_part(k):
        block = lk.at[pl.ds(k * MAT, MAT)]
        return copy(block, block, lsend.at[k], lrecv.at[k], (other, zt, xy))

    for k in range(2):
        pair_part(k).wait_recv()
        for c in range(k * PAIRS, (k + 1) * PAIRS):
            low, high = lk[other * half + c], lk[other * half + MAT + c]
            sx[0, pl.ds(other * MAT + c, 1)] = jnp.where(first, roll(low, 4, 0), high)[None]
            sx[1, pl.ds(other * MAT + c, 1)] = jnp.where(first, low, roll(high, 4, 0))[None]
            t_faces(other * MAT + c, low, high)
        for item in [up_face(other, k)] + t_copies(other, k):
            item.start()
        if k == 0:
            @pl.when(jnp.logical_not(at_bottom))
            def _():
                down_face(other, 0).start()
    for c in range(PAIRS):
        sx2[c] = jnp.where(first, lk[c], roll(lk[PAIRS + c], 4, 0))
    for c in range(MAT):
        cs_ll[c:c + 1] = lk[c][7:8]
        cs_ll[MAT + c:MAT + c + 1] = lk[3 * MAT + c][7:8]
        cs_hl[c:c + 1] = lk[3 * MAT + c][3:4]
        cs_lh[c:c + 1] = lk[c][4:5]
    rest = [
        copy(sx2, xtwo, lsend.at[4], lrecv.at[4], (g, zt, x_up)),
        copy(cs_ll, c_ll, lsend.at[5], lrecv.at[5], corner_dev[0]),
        copy(cs_lh, c_lh, lsend.at[6], lrecv.at[6], corner_dev[1]),
        copy(cs_hl, c_hl, lsend.at[7], lrecv.at[7], corner_dev[2]),
    ]
    for item in rest[:3]:
        item.start()

    @pl.when(at_bottom)
    def _():
        if near_barrier:
            pl.semaphore_wait(ready, len(above))
        below_near()
        down_face(other, 0).start()
    down_face(other, 1).start()
    rest[3].start()

    def pick(ref, c):
        return jnp.broadcast_to(ref[c:c + 1], (8, lanes))

    def widen(c, x, mine, low, high):
        between = jnp.where(late, low, high)
        return jnp.where(own, roll(mine, 2 - 4 * x, 0), roll(between, 6 - 4 * x, 0))

    def far_rows(block, low_corner, high_corner, x):
        row = jnp.where(own, roll(block, 2 - 4 * x, 0), 0.0)
        if low_corner is not None:
            row = jnp.where(sub == 1, low_corner, row)
        if high_corner is not None:
            row = jnp.where(sub == 6, high_corner, row)
        return row

    def extend(par, c):
        own_part = ws[par, c]
        corners = [jnp.broadcast_to(hb[par, 4 * COMPS + k, c:c + 1], (8, lanes)) for k in range(4)]
        x_lo, x_hi, t_lo, t_hi = [hb[par, k * COMPS + c] for k in range(4)]
        return [
            far_rows(x_lo, None, None, 0),
            far_rows(x_lo, corners[0], corners[1], 1),
            widen(c, 0, own_part, t_lo, t_hi),
            widen(c, 1, own_part, t_lo, t_hi),
            far_rows(x_hi, corners[2], corners[3], 0),
            far_rows(x_hi, None, None, 1),
        ]

    for item in scalars:
        item.wait()
    rows16 = lax.broadcasted_iota(jnp.int32, (16, lanes), 0)
    shift_rows = jnp.zeros((16, lanes), jnp.float32)
    residue_rows = jnp.zeros((16, lanes), jnp.float32)
    for k in range(nshift):
        shift_rows = jnp.where(rows16 == k, shifts_ref[k], shift_rows)
        residue_rows = jnp.where(rows16 == k, residues_ref[k], residue_rows)
    mass_sq = mass_ref[0] * mass_ref[0]

    for c in range(COMPS):
        rpack[c] = spack[c]
        out_ref[c] = jnp.zeros((8, lanes), jnp.float32)
        for k in range(nshift):
            shiftdirs[k, c] = spack[c]

    copy(st, tfar, lsend.at[3], lrecv.at[3], (g, t_up, xy)).wait()
    for k in range(2):
        pair_part(k).wait_send()

    t_at = lax.rem(zt * cells_t + sub - 2 + n_zt * cells_t, n_zt * cells_t)
    edge = jnp.where(t_at == n_zt * cells_t - 1, -0.5, 0.5)
    yz_sign = (1 - 2 * lax.rem(ycoord + zcoord, 2)).astype(jnp.float32)
    y_sign = (1 - 2 * lax.rem(ycoord, 2)).astype(jnp.float32)

    def z_up(v):
        cond = jnp.broadcast_to(zcoord == NZ - 1, v.shape)
        return jnp.where(cond, roll(v, NZ - 1, v.ndim - 1), roll(v, -1, v.ndim - 1))

    def z_dn(v):
        cond = jnp.broadcast_to(zcoord == 0, v.shape)
        return jnp.where(cond, roll(v, 1 - NZ, v.ndim - 1), roll(v, 1, v.ndim - 1))

    def wide_link(d, c, e):
        at = d * MAT + c
        sign = -1.0 if e % 2 else 1.0
        if e in (2, 3):
            low, high = tfar[0, (d // 2) * MAT + c], tfar[1, (d // 2) * MAT + c]
            if d % 2:
                low, high = roll(low, 2, 0), roll(high, -2, 0)
            value = widen(c, e - 2, lk[at], low, high)
        elif e == 0:
            value = far_rows(xtwo[c % PAIRS], None, None, c // PAIRS)
        elif e == 1:
            low = pick(c_ll, c) if d == 0 else (pick(c_ll, MAT + c) if d == 3 else None)
            value = far_rows(xfar[0, (d // 2) * MAT + c], low, pick(c_lh, c) if d == 0 else None, d % 2)
        else:
            value = far_rows(xfar[1, (d // 2) * MAT + c], pick(c_hl, c) if d == 3 else None, None, d % 2)
        if d == 0:
            return 0.5 * value
        if d == 1:
            return (0.5 * sign) * value
        if d == 2:
            return (0.5 * sign) * y_sign * value
        return sign * yz_sign * edge * value

    def build(rows):
        for part_no in range(2):
            for i in range(3):
                for j in range(3):
                    c = part_no * PAIRS + i * 3 + j
                    flip = part_no * PAIRS + j * 3 + i
                    back = 1.0 if part_no else -1.0
                    for e in rows:
                        wx = wide_link(0, c, e)
                        if e > 0:
                            gauge[0, c, e - 1] = wx
                        if e < 4:
                            gauge[1, flip, e] = back * wx
                        if e == 0:
                            continue
                        wz = wide_link(2, c, e)
                        gauge[3, c, e - 1] = wz
                        gauge[4, flip, e - 1] = back * z_dn(wz)
                        wt = wide_link(3, c, e)
                        gauge[5, c, e - 1] = wt
                        gauge[6, flip, e - 1] = back * roll(wt, 1, 0)
                        wy = wide_link(1, c, e)
                        turned = wide_link(1, flip, e)
                        gauge[2, c, e - 1] = wy + back * roll(turned, NZ, 1)

    build((2, 3))
    for item in [copy(sx, xfar, lsend.at[2], lrecv.at[2], (g, zt, x_up))] + rest:
        item.wait()
    build((0, 1, 4))

    def finish_halo(par):
        copy(hb.at[par], hb.at[par], hsend.at[par], hrecv.at[par], corner_dev[0]).wait()

    finish_halo(0)

    def hop(field, e0):
        total = [None] * COMPS
        terms = (
            (0, lambda c: field[c, e0 + 1:e0 + 3]),
            (1, lambda c: field[c, e0 - 1:e0 + 1]),
            (2, lambda c: roll(field[c, e0:e0 + 2], NZ, 2)),
            (3, lambda c: z_up(field[c, e0:e0 + 2])),
            (4, lambda c: z_dn(field[c, e0:e0 + 2])),
            (5, lambda c: roll(field[c, e0:e0 + 2], -1, 1)),
            (6, lambda c: roll(field[c, e0:e0 + 2], 1, 1)),
        )
        for term, shifted in terms:
            v = [shifted(c) for c in range(COMPS)]
            for i in range(3):
                for j in range(3):
                    wre = gauge[term, i * 3 + j, e0 - 1:e0 + 1]
                    wim = gauge[term, PAIRS + i * 3 + j, e0 - 1:e0 + 1]
                    re = wre * v[j] - wim * v[3 + j]
                    im = wre * v[3 + j] + wim * v[j]
                    total[i] = re if total[i] is None else total[i] + re
                    total[3 + i] = im if total[3 + i] is None else total[3 + i] + im
        return total

    def hop_wide(par):
        for c in range(COMPS):
            for e, value in enumerate(extend(par, c)):
                wide[c, e] = value
        for e0 in (1, 3):
            for c, value in enumerate(hop(wide, e0)):
                hop_w[c, e0:e0 + 2] = value

    hop_wide(0)
    for c in range(COMPS):
        dpack_ref[c] = spack[c]
        hop_r[c, 1:5] = hop_w[c, 1:5]
        mid[c, 1:5] = hop_w[c, 1:5]

    def image_of():
        image = hop(mid, 2)
        packed = []
        for c in range(COMPS):
            wp = jnp.where(first, roll(image[c][0], -2, 0), roll(image[c][1], 2, 0))
            packed.append(mass_sq * dpack_ref[c] - wp)
        return packed, [dpack_ref[c] for c in range(COMPS)]

    def row(values, k):
        return jnp.broadcast_to(values[k:k + 1], (8, lanes))

    def accumulate(gain):
        for c in range(COMPS):
            total = out_ref[c]
            for k in range(nshift):
                total = total + row(gain, k) * shiftdirs[k, c]
            out_ref[c] = total

    def catch_up(gain, zeta_now, beta_shift):
        accumulate(gain)
        for k in range(nshift):
            zk, bk = row(zeta_now, k), row(beta_shift, k)
            for c in range(COMPS):
                shiftdirs[k, c] = zk * rpack[c] + bk * shiftdirs[k, c]

    lane16 = lax.broadcasted_iota(jnp.int32, (16, lanes), 1)
    swap = copy(mine, theirs, asend.at[1], arecv.at[1], (other, zt, xy))

    def closing(sums, values):
        norm, zeta, zeta_old, alpha_old, beta_old, beta_shift, along, score = values
        alpha = norm / fill(sums, 0)
        zeta_new = zeta * zeta_old * alpha_old / (
            alpha * beta_old * (zeta_old - zeta) + zeta_old * alpha_old * (1.0 + shift_rows * alpha)
        )
        gain = residue_rows * alpha * (zeta_new / zeta)
        return gain, score + gain * (zeta * fill(sums, 3) + beta_shift * along)

    def iterate(step, last):
        norm, zeta, zeta_old, alpha_old, beta_old, beta_shift, along, score, gain = [state[k] for k in range(9)]
        par = step % 2 if last else lax.rem(step, 2)
        if last:
            packed_state = norm
            for k in range(1, 8):
                packed_state = jnp.where(lane16 == k, state[k], packed_state)
            mine[...] = packed_state
            swap.start()
        packed, dpack = image_of()
        res = [rpack[c] for c in range(COMPS)]
        part[par, pl.ds(me, 1)] = dots([inner(dpack, packed), inner(res, packed), inner(packed, packed), inner(spack, res)])[None]
        send_part(par)
        if last:
            send_cross(par)
        else:
            corner_tiles(packed, par)
            for c in range(COMPS):
                ws[par, c] = packed[c]
            start_halo(par)
        catch_up(gain, zeta, beta_shift)
        if not last:
            finish_halo(par)
            hop_wide(par)
        wait_part(par)
        sums = summed(lambda j: part[par, j])
        if last:
            gain, score = closing(sums, [state[k] for k in range(8)])
            accumulate(gain)
            return score
        norm = jnp.where(step == 1, fill(sums, 3), norm)
        alpha = norm / fill(sums, 0)
        zeta_new = zeta * zeta_old * alpha_old / (
            alpha * beta_old * (zeta_old - zeta) + zeta_old * alpha_old * (1.0 + shift_rows * alpha)
        )
        ratio = zeta_new / zeta
        along = zeta * fill(sums, 3) + beta_shift * along
        gain = residue_rows * alpha * ratio
        score = score + gain * along
        norm_next = norm - 2.0 * alpha * fill(sums, 1) + alpha * alpha * fill(sums, 2)
        beta = norm_next / norm
        beta_shift = beta * ratio * ratio
        step_a, step_b = row(alpha, 0), row(beta, 0)
        for c in range(COMPS):
            fresh = rpack[c] - step_a * ws[par, c]
            rpack[c] = fresh
            dpack_ref[c] = fresh + step_b * dpack_ref[c]
            for e in range(1, 5):
                fresh = hop_r[c, e] - step_a * hop_w[c, e]
                hop_r[c, e] = fresh
                mid[c, e] = fresh + step_b * mid[c, e]
        for k, value in enumerate((norm_next, zeta_new, zeta, alpha, beta, beta_shift, along, score, gain)):
            state[k] = value

    one = jnp.ones((16, lanes), jnp.float32)
    none = jnp.zeros((16, lanes), jnp.float32)

    def body(step, carry):
        iterate(step, False)
        return carry

    for k, value in enumerate((one, one, one, one, none, none, none, none, none)):
        state[k] = value
    lax.fori_loop(1, ITERS, body, 0)
    score = iterate(ITERS, True)
    swap.wait()
    copy(cross, cross, asend.at[0], arecv.at[0], corner_dev[0]).wait()
    far_state = theirs[...]
    values = [jnp.broadcast_to(far_state[:, k:k + 1], (16, lanes)) for k in range(8)]
    total = score + closing(summed(lambda j: cross[j]), values)[1]
    sites = n_grp * n_all * cells_x * cells_t * lanes
    action_ref[0] = jnp.max(jnp.sum(total, axis=0, keepdims=True)) * (1.0 / sites)


def on_device(sizes, source, links, shifts, residues, mass):
    n_grp, n_zt, n_xy = sizes
    cells_x, cells_t, lanes = source.shape[3:]
    n_all = n_zt * n_xy
    f32 = jnp.float32
    tiles = lambda *lead: pltpu.VMEM(lead + (8, lanes), f32)
    rows = lambda count: pltpu.VMEM((count, lanes), f32)
    nshift = shifts.shape[0]
    vmem = pl.BlockSpec(memory_space=pltpu.VMEM)
    smem = pl.BlockSpec(memory_space=pltpu.SMEM)
    dma = pltpu.SemaphoreType.DMA
    rational, action = pl.pallas_call(
        functools.partial(kernel, (n_grp, n_zt, n_xy, cells_x, cells_t)),
        out_shape=(
            pltpu.VMEM((COMPS, 8, lanes), f32),
            pltpu.SMEM((1,), f32),
        ),
        in_specs=[pl.BlockSpec(memory_space=pltpu.HBM)] * 5,
        out_specs=(vmem, smem),
        scratch_shapes=[
            tiles(4 * MAT), tiles(2, 2 * MAT), tiles(2, 2 * MAT), tiles(PAIRS), tiles(2, 2 * MAT), tiles(2, 2 * MAT), tiles(PAIRS),
            rows(40), rows(24), rows(24), rows(40), rows(24), rows(24),
            tiles(7, MAT, 4), tiles(COMPS, 6), tiles(COMPS, 6), tiles(COMPS, 6), tiles(COMPS, 6), tiles(COMPS),
            tiles(nshift, COMPS), tiles(COMPS), tiles(2, COMPS), tiles(2, 4), tiles(2, 4 * COMPS + 4),
            pltpu.VMEM((2, n_all, 1, lanes), f32), pltpu.VMEM((n_all, 1, lanes), f32),
            pltpu.VMEM((9, 16, lanes), f32), rows(16), rows(16), tiles(COMPS), tiles(2 * MAT),
            pltpu.SMEM((nshift,), f32), pltpu.SMEM((nshift,), f32), pltpu.SMEM((1,), f32), dma((5,)),
            dma((8,)), dma((8,)), dma((2,)), dma((2,)), dma((2,)), dma((2,)), dma((2,)), dma((2,)),
            pltpu.SemaphoreType.REGULAR,
        ],
        compiler_params=pltpu.CompilerParams(collective_id=0, has_side_effects=True),
    )(
        source.reshape(COMPS, 8, lanes), links.reshape(2 * MAT, 8, lanes), shifts, residues, mass
    )
    return rational.reshape(source.shape), action


def solution(mesh):
    sizes = tuple(mesh.shape[name] for name in ("grp", "zt", "xy"))
    field = P("grp", None, None, "xy", "zt", None)
    return jax.shard_map(
        functools.partial(on_device, sizes),
        mesh=mesh,
        in_specs=(field, P("grp", None, None, None, "xy", "zt", None), P(), P(), P()),
        out_specs=(field, P()),
        check_vma=False,
    )
```

```python
import functools

import jax
import jax.numpy as jnp
from jax import lax
from jax.experimental import pallas as pl
from jax.experimental.pallas import tpu as pltpu
from jax.sharding import PartitionSpec as P

NY = 2
NZ = 64
ITERS = 8
PAIRS = 9
MAT = 2 * PAIRS
COMPS = 6


def roll(value, shift, axis):
    size = value.shape[axis]
    return pltpu.roll(value, shift % size, axis)


def kernel(
    dims, source_hbm, links_hbm, shifts_hbm, residues_hbm, mass_hbm, out_ref, action_ref,
    lk, tfar, xfar, xtwo, sx, st, sx2, cs_ll, cs_hl, cs_lh, c_ll, c_hl, c_lh,
    gauge, wide, hop_w, hop_r, mid, dpack_ref, shiftdirs, rpack, ws, cs, hb, part, cross,
    state, mine, theirs, source_ref, links_ref, shifts_ref, residues_ref, mass_ref,
    isem, lsend, lrecv, hsend, hrecv, psend, precv, asend, arecv, ready,
):
    n_grp, n_zt, n_xy, cells_x, cells_t = dims
    lanes = NY * NZ
    n_all = n_zt * n_xy
    nshift = shifts_ref.shape[0]
    g = lax.axis_index("grp")
    zt = lax.axis_index("zt")
    xy = lax.axis_index("xy")
    me = zt * n_xy + xy
    me_all = g * n_all + me
    x_up, x_dn = lax.rem(xy + 1, n_xy), lax.rem(xy + n_xy - 1, n_xy)
    t_up, t_dn = lax.rem(zt + 1, n_zt), lax.rem(zt + n_zt - 1, n_zt)
    other = 1 - g

    def place(linear):
        inside = lax.rem(linear, n_all)
        return (linear // n_all, inside // n_xy, lax.rem(inside, n_xy))

    def each(count, fn):
        if count <= 32:
            for p in range(1, count):
                fn(p)
        else:
            def step(p, carry):
                fn(p)
                return carry
            lax.fori_loop(1, count, step, 0)

    def copy(src, dst, send, recv, device):
        return pltpu.make_async_remote_copy(
            src_ref=src, dst_ref=dst, send_sem=send, recv_sem=recv,
            device_id=device, device_id_type=pl.DeviceIdType.MESH,
        )

    barrier = pltpu.get_barrier_semaphore()

    corner_dev = ((g, t_up, x_up), (g, t_dn, x_up), (g, t_up, x_dn), (g, t_dn, x_dn))
    above = ((g, zt, x_up),) + corner_dev[:2]
    partners = ((other, zt, xy), (g, t_up, xy), (g, t_dn, xy), (g, zt, x_dn)) + corner_dev[2:]
    near_barrier = n_zt <= 4 and n_xy <= 4
    at_top, at_bottom = xy == n_xy - 1, xy == 0

    def greet(device):
        pl.semaphore_signal(barrier, inc=1, device_id=device, device_id_type=pl.DeviceIdType.MESH)

    fetch_links = pltpu.make_async_copy(links_hbm, links_ref, isem.at[0])
    fetch_source = pltpu.make_async_copy(source_hbm, source_ref, isem.at[1])
    if near_barrier:
        for device in partners:
            greet(device)

        @pl.when(jnp.logical_not(at_top))
        def _():
            for device in above:
                greet(device)
    else:
        each(n_grp * n_all, lambda p: greet(place(lax.rem(me_all + p, n_grp * n_all))))
    fetch_links.start()
    fetch_source.start()
    scalars = [
        pltpu.make_async_copy(src, dst, isem.at[2 + k])
        for k, (src, dst) in enumerate(((shifts_hbm, shifts_ref), (residues_hbm, residues_ref), (mass_hbm, mass_ref)))
    ]
    for item in scalars:
        item.start()
    fetch_links.wait()
    fetch_source.wait()

    sub = lax.broadcasted_iota(jnp.int32, (8, lanes), 0)
    lane = lax.broadcasted_iota(jnp.int32, (8, lanes), 1)
    zcoord = lax.rem(lane, NZ)
    ycoord = lane // NZ
    quarter = lanes // 4
    home = sub == lane // quarter
    own = (sub >= 2) & (sub < 2 + cells_t)
    first = sub < cells_t
    late = lax.rem(sub, cells_t) >= 2

    def t_faces(c, one, two):
        st[0, pl.ds(c, 1)] = jnp.where(late, one, roll(two, -2, 0))[None]
        st[1, pl.ds(c, 1)] = jnp.where(late, roll(two, 2, 0), one)[None]

    for d in range(2):
        for c in range(MAT):
            low, high = links_ref[c], links_ref[MAT + c]
            if d == 0:
                sx[0, pl.ds(g * MAT + c, 1)] = jnp.where(first, roll(low, 4, 0), high)[None]
            else:
                sx[1, pl.ds(g * MAT + c, 1)] = jnp.where(first, low, roll(high, 4, 0))[None]
    for c in range(MAT):
        t_faces(g * MAT + c, links_ref[c], links_ref[MAT + c])
    for c in range(2 * MAT):
        lk[pl.ds(g * 2 * MAT + c, 1)] = links_ref[c][None]

    spack = [source_ref[c] for c in range(COMPS)]

    def corner_tiles(tiles, par):
        for k, row in enumerate((7, 4, 3, 0)):
            tile = jnp.zeros((8, lanes), jnp.float32)
            for c in range(COMPS):
                tile = jnp.where(sub == c, jnp.broadcast_to(tiles[c][row:row + 1], (8, lanes)), tile)
            cs[par, k] = tile

    def face(par, k):
        device = ((g, zt, x_up), (g, zt, x_dn), (g, t_up, xy), (g, t_dn, xy))[k]
        at = k * COMPS if k < 2 else k * COMPS + 4
        return copy(ws.at[par], hb.at[par, pl.ds(at, COMPS)], hsend.at[par], hrecv.at[par, k // 2], device)

    def corner(par, k):
        return copy(cs.at[par, pl.ds(k, 1)], hb.at[par, pl.ds(2 * COMPS + k, 1)], hsend.at[par], hrecv.at[par, 0], corner_dev[k])

    def start_faces(par):
        @pl.when(at_bottom)
        def _():
            face(par, 1).start()
        face(par, 0).start()

        @pl.when(jnp.logical_not(at_bottom))
        def _():
            face(par, 1).start()
        face(par, 2).start()
        face(par, 3).start()

    def start_corners(par):
        for k in range(4):
            corner(par, k).start()

    def send_part(par):
        def go(p):
            copy(part.at[par, me], part.at[par, me], psend.at[par], precv.at[par],
                 (g,) + place(lax.rem(me + p, n_all))[1:]).start()
        each(n_all, go)

    def wait_part(par):
        rest = part.at[par, pl.ds(0, n_all - 1)]
        copy(rest, rest, psend.at[par], precv.at[par], corner_dev[0]).wait()

    def send_cross(par):
        def go(p):
            copy(part.at[par, me], cross.at[me], asend.at[0], arecv.at[0],
                 (other,) + place(lax.rem(me + p, n_all))[1:]).start()
        go(0)
        each(n_all, go)

    def dots(rows):
        tile = jnp.zeros((8, lanes), jnp.float32)
        for k, row in enumerate(rows):
            tile = jnp.where(sub == k, jnp.broadcast_to(jnp.sum(row, axis=0, keepdims=True), (8, lanes)), tile)
        tile = (tile + roll(tile, 2 * quarter, 1)) + (roll(tile, quarter, 1) + roll(tile, 3 * quarter, 1))
        return jnp.sum(jnp.where(home, tile, 0.0), axis=0, keepdims=True)

    def summed(row_of):
        if n_all <= 32:
            level = [row_of(j) for j in range(n_all)]
            while len(level) > 1:
                odd = level[len(level) // 2 * 2:]
                level = [level[k] + level[k + 1] for k in range(0, len(level) - 1, 2)] + odd
            total = level[0]
        else:
            total = lax.fori_loop(1, n_all, lambda j, acc: acc + row_of(j), row_of(0))
        split = jnp.where(home, jnp.broadcast_to(total, (8, lanes)), 0.0)
        return jnp.broadcast_to(jnp.sum(split, axis=1, keepdims=True), (8, lanes))

    def fill(values, k):
        return jnp.broadcast_to(values[k:k + 1], (16, lanes))

    def inner(left, right):
        total = left[0] * right[0]
        for c in range(1, COMPS):
            total = total + left[c] * right[c]
        return total

    corner_tiles(spack, 0)
    for c in range(COMPS):
        ws[0, c] = spack[c]

    if near_barrier:
        pl.semaphore_wait(barrier, len(partners) + jnp.where(at_bottom, 0, len(above)))

        @pl.when(at_top)
        def _():
            for device in above:
                pl.semaphore_signal(ready, inc=1, device_id=device, device_id_type=pl.DeviceIdType.MESH)
    else:
        pl.semaphore_wait(barrier, n_grp * n_all - 1)

    half = 2 * MAT

    def to_pair(k):
        found = []
        for d in range(2):
            span = d * MAT + k * PAIRS
            found.append(copy(
                links_ref.at[pl.ds(span, PAIRS)], lk.at[pl.ds(g * half + span, PAIRS)],
                lsend.at[k], lrecv.at[k], (other, zt, xy),
            ))
        return found

    def span_of(h, k):
        return pl.ds(h * MAT + k * PAIRS, PAIRS)

    def up_face(h, k):
        span = span_of(h, k)
        return copy(sx.at[0, span], xfar.at[0, span], lsend.at[2], lrecv.at[2], (g, zt, x_up))

    def down_face(h, k):
        span = span_of(h, k)
        return copy(sx.at[1, span], xfar.at[1, span], lsend.at[2], lrecv.at[2], (g, zt, x_dn))

    def t_copies(h, k):
        span = span_of(h, k)
        return [
            copy(st.at[0, span], tfar.at[0, span], lsend.at[3], lrecv.at[3], (g, t_up, xy)),
            copy(st.at[1, span], tfar.at[1, span], lsend.at[3], lrecv.at[3], (g, t_dn, xy)),
        ]

    def below_near():
        for k in range(2):
            down_face(g, k).start()
        for k in (2, 3):
            corner(0, k).start()
        face(0, 1).start()

    for k in range(2):
        for item in to_pair(k):
            item.start()
    for k in range(2):
        for item in [up_face(g, k)] + t_copies(g, k):
            item.start()
    for k in (0, 1):
        corner(0, k).start()
    for k in (0, 2, 3):
        face(0, k).start()

    @pl.when(jnp.logical_not(at_bottom))
    def _():
        below_near()

    def pair_part(k):
        block = lk.at[pl.ds(k * MAT, MAT)]
        return copy(block, block, lsend.at[k], lrecv.at[k], (other, zt, xy))

    for k in range(2):
        pair_part(k).wait_recv()
        for c in range(k * PAIRS, (k + 1) * PAIRS):
            low, high = lk[other * half + c], lk[other * half + MAT + c]
            sx[0, pl.ds(other * MAT + c, 1)] = jnp.where(first, roll(low, 4, 0), high)[None]
            sx[1, pl.ds(other * MAT + c, 1)] = jnp.where(first, low, roll(high, 4, 0))[None]
            t_faces(other * MAT + c, low, high)
        for item in [up_face(other, k)] + t_copies(other, k):
            item.start()
        if k == 0:
            @pl.when(jnp.logical_not(at_bottom))
            def _():
                down_face(other, 0).start()
    for c in range(PAIRS):
        sx2[c] = jnp.where(first, lk[c], roll(lk[PAIRS + c], 4, 0))
    for c in range(MAT):
        cs_ll[c:c + 1] = lk[c][7:8]
        cs_ll[MAT + c:MAT + c + 1] = lk[3 * MAT + c][7:8]
        cs_hl[c:c + 1] = lk[3 * MAT + c][3:4]
        cs_lh[c:c + 1] = lk[c][4:5]
    rest = [
        copy(sx2, xtwo, lsend.at[4], lrecv.at[4], (g, zt, x_up)),
        copy(cs_ll, c_ll, lsend.at[5], lrecv.at[5], corner_dev[0]),
        copy(cs_lh, c_lh, lsend.at[6], lrecv.at[6], corner_dev[1]),
        copy(cs_hl, c_hl, lsend.at[7], lrecv.at[7], corner_dev[2]),
    ]
    for item in rest[:3]:
        item.start()

    @pl.when(at_bottom)
    def _():
        if near_barrier:
            pl.semaphore_wait(ready, len(above))
        below_near()
        down_face(other, 0).start()
    down_face(other, 1).start()
    rest[3].start()

    def pick(ref, c):
        return jnp.broadcast_to(ref[c:c + 1], (8, lanes))

    def widen(c, x, mine, low, high):
        between = jnp.where(late, low, high)
        return jnp.where(own, roll(mine, 2 - 4 * x, 0), roll(between, 6 - 4 * x, 0))

    def far_rows(block, low_corner, high_corner, x):
        row = jnp.where(own, roll(block, 2 - 4 * x, 0), 0.0)
        if low_corner is not None:
            row = jnp.where(sub == 1, low_corner, row)
        if high_corner is not None:
            row = jnp.where(sub == 6, high_corner, row)
        return row

    def extend_t(par, c):
        t_lo, t_hi = hb[par, 2 * COMPS + 4 + c], hb[par, 3 * COMPS + 4 + c]
        for x in range(2):
            wide[c, 2 + x] = widen(c, x, ws[par, c], t_lo, t_hi)

    def extend_x(par, c):
        corners = [jnp.broadcast_to(hb[par, 2 * COMPS + k, c:c + 1], (8, lanes)) for k in range(4)]
        x_lo, x_hi = hb[par, c], hb[par, COMPS + c]
        wide[c, 0] = far_rows(x_lo, None, None, 0)
        wide[c, 1] = far_rows(x_lo, corners[0], corners[1], 1)
        wide[c, 4] = far_rows(x_hi, corners[2], corners[3], 0)
        wide[c, 5] = far_rows(x_hi, None, None, 1)

    for item in scalars:
        item.wait()
    rows16 = lax.broadcasted_iota(jnp.int32, (16, lanes), 0)
    shift_rows = jnp.zeros((16, lanes), jnp.float32)
    residue_rows = jnp.zeros((16, lanes), jnp.float32)
    for k in range(nshift):
        shift_rows = jnp.where(rows16 == k, shifts_ref[k], shift_rows)
        residue_rows = jnp.where(rows16 == k, residues_ref[k], residue_rows)
    mass_sq = mass_ref[0] * mass_ref[0]

    for c in range(COMPS):
        rpack[c] = spack[c]
        out_ref[c] = jnp.zeros((8, lanes), jnp.float32)
        for k in range(nshift):
            shiftdirs[k, c] = spack[c]

    copy(st, tfar, lsend.at[3], lrecv.at[3], (g, t_up, xy)).wait()
    for k in range(2):
        pair_part(k).wait_send()

    t_at = lax.rem(zt * cells_t + sub - 2 + n_zt * cells_t, n_zt * cells_t)
    edge = jnp.where(t_at == n_zt * cells_t - 1, -0.5, 0.5)
    yz_sign = (1 - 2 * lax.rem(ycoord + zcoord, 2)).astype(jnp.float32)
    y_sign = (1 - 2 * lax.rem(ycoord, 2)).astype(jnp.float32)

    def z_up(v):
        cond = jnp.broadcast_to(zcoord == NZ - 1, v.shape)
        return jnp.where(cond, roll(v, NZ - 1, v.ndim - 1), roll(v, -1, v.ndim - 1))

    def z_dn(v):
        cond = jnp.broadcast_to(zcoord == 0, v.shape)
        return jnp.where(cond, roll(v, 1 - NZ, v.ndim - 1), roll(v, 1, v.ndim - 1))

    def wide_link(d, c, e):
        at = d * MAT + c
        sign = -1.0 if e % 2 else 1.0
        if e in (2, 3):
            low, high = tfar[0, (d // 2) * MAT + c], tfar[1, (d // 2) * MAT + c]
            if d % 2:
                low, high = roll(low, 2, 0), roll(high, -2, 0)
            value = widen(c, e - 2, lk[at], low, high)
        elif e == 0:
            value = far_rows(xtwo[c % PAIRS], None, None, c // PAIRS)
        elif e == 1:
            low = pick(c_ll, c) if d == 0 else (pick(c_ll, MAT + c) if d == 3 else None)
            value = far_rows(xfar[0, (d // 2) * MAT + c], low, pick(c_lh, c) if d == 0 else None, d % 2)
        else:
            value = far_rows(xfar[1, (d // 2) * MAT + c], pick(c_hl, c) if d == 3 else None, None, d % 2)
        if d == 0:
            return 0.5 * value
        if d == 1:
            return (0.5 * sign) * value
        if d == 2:
            return (0.5 * sign) * y_sign * value
        return sign * yz_sign * edge * value

    def build(rows):
        for part_no in range(2):
            for i in range(3):
                for j in range(3):
                    c = part_no * PAIRS + i * 3 + j
                    flip = part_no * PAIRS + j * 3 + i
                    back = 1.0 if part_no else -1.0
                    for e in rows:
                        wx = wide_link(0, c, e)
                        if e > 0:
                            gauge[0, c, e - 1] = wx
                        if e < 4:
                            gauge[1, flip, e] = back * wx
                        if e == 0:
                            continue
                        wz = wide_link(2, c, e)
                        gauge[3, c, e - 1] = wz
                        gauge[4, flip, e - 1] = back * z_dn(wz)
                        wt = wide_link(3, c, e)
                        gauge[5, c, e - 1] = wt
                        gauge[6, flip, e - 1] = back * roll(wt, 1, 0)
                        wy = wide_link(1, c, e)
                        turned = wide_link(1, flip, e)
                        gauge[2, c, e - 1] = wy + back * roll(turned, NZ, 1)

    build((2, 3))
    for item in [copy(sx, xfar, lsend.at[2], lrecv.at[2], (g, zt, x_up))] + rest:
        item.wait()
    build((0, 1, 4))

    def wait_x(par):
        block = hb.at[par, pl.ds(0, 2 * COMPS + 4)]
        copy(block, block, hsend.at[par], hrecv.at[par, 0], corner_dev[0]).wait_recv()

    def wait_t(par):
        block = hb.at[par, pl.ds(2 * COMPS + 4, 2 * COMPS)]
        copy(block, block, hsend.at[par], hrecv.at[par, 1], corner_dev[0]).wait_recv()

    def wait_sent(par):
        copy(hb.at[par], hb.at[par], hsend.at[par], hrecv.at[par, 0], corner_dev[0]).wait_send()

    def hop(field, e0, count, terms, total):
        shifts_of = (
            lambda c: field[c, e0 + 1:e0 + 1 + count],
            lambda c: field[c, e0 - 1:e0 - 1 + count],
            lambda c: roll(field[c, e0:e0 + count], NZ, 2),
            lambda c: z_up(field[c, e0:e0 + count]),
            lambda c: z_dn(field[c, e0:e0 + count]),
            lambda c: roll(field[c, e0:e0 + count], -1, 1),
            lambda c: roll(field[c, e0:e0 + count], 1, 1),
        )
        for term in terms:
            v = [shifts_of[term](c) for c in range(COMPS)]
            for i in range(3):
                for j in range(3):
                    wre = gauge[term, i * 3 + j, e0 - 1:e0 - 1 + count]
                    wim = gauge[term, PAIRS + i * 3 + j, e0 - 1:e0 - 1 + count]
                    re = wre * v[j] - wim * v[3 + j]
                    im = wre * v[3 + j] + wim * v[j]
                    total[i] = re if total[i] is None else total[i] + re
                    total[3 + i] = im if total[3 + i] is None else total[3 + i] + im
        return total

    every = tuple(range(7))

    def hop_wide(par):
        wait_t(par)
        for c in range(COMPS):
            extend_t(par, c)
        for c, value in enumerate(hop(wide, 2, 2, every[2:], [None] * COMPS)):
            hop_w[c, 2:4] = value
        wait_x(par)
        for c in range(COMPS):
            extend_x(par, c)
        for c, value in enumerate(hop(wide, 2, 2, every[:2], [hop_w[c, 2:4] for c in range(COMPS)])):
            hop_w[c, 2:4] = value
        for e in (1, 4):
            for c, value in enumerate(hop(wide, e, 1, every, [None] * COMPS)):
                hop_w[c, e:e + 1] = value
        wait_sent(par)

    hop_wide(0)
    for c in range(COMPS):
        dpack_ref[c] = spack[c]
        hop_r[c, 1:5] = hop_w[c, 1:5]
        mid[c, 1:5] = hop_w[c, 1:5]

    def image_of():
        image = hop(mid, 2, 2, every, [None] * COMPS)
        packed = []
        for c in range(COMPS):
            wp = jnp.where(first, roll(image[c][0], -2, 0), roll(image[c][1], 2, 0))
            packed.append(mass_sq * dpack_ref[c] - wp)
        return packed, [dpack_ref[c] for c in range(COMPS)]

    def row(values, k):
        return jnp.broadcast_to(values[k:k + 1], (8, lanes))

    def accumulate(gain):
        for c in range(COMPS):
            total = out_ref[c]
            for k in range(nshift):
                total = total + row(gain, k) * shiftdirs[k, c]
            out_ref[c] = total

    def catch_up(gain, zeta_now, beta_shift):
        accumulate(gain)
        for k in range(nshift):
            zk, bk = row(zeta_now, k), row(beta_shift, k)
            for c in range(COMPS):
                shiftdirs[k, c] = zk * rpack[c] + bk * shiftdirs[k, c]

    lane16 = lax.broadcasted_iota(jnp.int32, (16, lanes), 1)
    swap = copy(mine, theirs, asend.at[1], arecv.at[1], (other, zt, xy))

    def closing(sums, values):
        norm, zeta, zeta_old, alpha_old, beta_old, beta_shift, along, score = values
        alpha = norm / fill(sums, 0)
        zeta_new = zeta * zeta_old * alpha_old / (
            alpha * beta_old * (zeta_old - zeta) + zeta_old * alpha_old * (1.0 + shift_rows * alpha)
        )
        gain = residue_rows * alpha * (zeta_new / zeta)
        return gain, score + gain * (zeta * fill(sums, 3) + beta_shift * along)

    def iterate(step, last):
        norm, zeta, zeta_old, alpha_old, beta_old, beta_shift, along, score, gain = [state[k] for k in range(9)]
        par = step % 2 if last else lax.rem(step, 2)
        if last:
            packed_state = norm
            for k in range(1, 8):
                packed_state = jnp.where(lane16 == k, state[k], packed_state)
            mine[...] = packed_state
            swap.start()
        packed, dpack = image_of()
        if not last:
            corner_tiles(packed, par)
            start_corners(par)
            for c in range(COMPS):
                ws[par, c] = packed[c]
        res = [rpack[c] for c in range(COMPS)]
        part[par, pl.ds(me, 1)] = dots([inner(dpack, packed), inner(res, packed), inner(packed, packed), inner(spack, res)])[None]
        send_part(par)
        if last:
            send_cross(par)
        else:
            start_faces(par)
        catch_up(gain, zeta, beta_shift)
        if not last:
            hop_wide(par)
        wait_part(par)
        sums = summed(lambda j: part[par, j])
        if last:
            gain, score = closing(sums, [state[k] for k in range(8)])
            accumulate(gain)
            return score
        norm = jnp.where(step == 1, fill(sums, 3), norm)
        alpha = norm / fill(sums, 0)
        zeta_new = zeta * zeta_old * alpha_old / (
            alpha * beta_old * (zeta_old - zeta) + zeta_old * alpha_old * (1.0 + shift_rows * alpha)
        )
        ratio = zeta_new / zeta
        along = zeta * fill(sums, 3) + beta_shift * along
        gain = residue_rows * alpha * ratio
        score = score + gain * along
        norm_next = norm - 2.0 * alpha * fill(sums, 1) + alpha * alpha * fill(sums, 2)
        beta = norm_next / norm
        beta_shift = beta * ratio * ratio
        step_a, step_b = row(alpha, 0), row(beta, 0)
        for c in range(COMPS):
            fresh = rpack[c] - step_a * ws[par, c]
            rpack[c] = fresh
            dpack_ref[c] = fresh + step_b * dpack_ref[c]
            for e in range(1, 5):
                fresh = hop_r[c, e] - step_a * hop_w[c, e]
                hop_r[c, e] = fresh
                mid[c, e] = fresh + step_b * mid[c, e]
        for k, value in enumerate((norm_next, zeta_new, zeta, alpha, beta, beta_shift, along, score, gain)):
            state[k] = value

    one = jnp.ones((16, lanes), jnp.float32)
    none = jnp.zeros((16, lanes), jnp.float32)

    def body(step, carry):
        iterate(step, False)
        return carry

    for k, value in enumerate((one, one, one, one, none, none, none, none, none)):
        state[k] = value
    lax.fori_loop(1, ITERS, body, 0)
    score = iterate(ITERS, True)
    swap.wait()
    copy(cross, cross, asend.at[0], arecv.at[0], corner_dev[0]).wait()
    far_state = theirs[...]
    values = [jnp.broadcast_to(far_state[:, k:k + 1], (16, lanes)) for k in range(8)]
    total = score + closing(summed(lambda j: cross[j]), values)[1]
    sites = n_grp * n_all * cells_x * cells_t * lanes
    action_ref[0] = jnp.max(jnp.sum(total, axis=0, keepdims=True)) * (1.0 / sites)


def on_device(sizes, source, links, shifts, residues, mass):
    n_grp, n_zt, n_xy = sizes
    cells_x, cells_t, lanes = source.shape[3:]
    n_all = n_zt * n_xy
    f32 = jnp.float32
    tiles = lambda *lead: pltpu.VMEM(lead + (8, lanes), f32)
    rows = lambda count: pltpu.VMEM((count, lanes), f32)
    nshift = shifts.shape[0]
    vmem = pl.BlockSpec(memory_space=pltpu.VMEM)
    smem = pl.BlockSpec(memory_space=pltpu.SMEM)
    dma = pltpu.SemaphoreType.DMA
    rational, action = pl.pallas_call(
        functools.partial(kernel, (n_grp, n_zt, n_xy, cells_x, cells_t)),
        out_shape=(
            pltpu.VMEM((COMPS, 8, lanes), f32),
            pltpu.SMEM((1,), f32),
        ),
        in_specs=[pl.BlockSpec(memory_space=pltpu.HBM)] * 5,
        out_specs=(vmem, smem),
        scratch_shapes=[
            tiles(4 * MAT), tiles(2, 2 * MAT), tiles(2, 2 * MAT), tiles(PAIRS), tiles(2, 2 * MAT), tiles(2, 2 * MAT), tiles(PAIRS),
            rows(40), rows(24), rows(24), rows(40), rows(24), rows(24),
            tiles(7, MAT, 4), tiles(COMPS, 6), tiles(COMPS, 6), tiles(COMPS, 6), tiles(COMPS, 6), tiles(COMPS),
            tiles(nshift, COMPS), tiles(COMPS), tiles(2, COMPS), tiles(2, 4), tiles(2, 4 * COMPS + 4),
            pltpu.VMEM((2, n_all, 1, lanes), f32), pltpu.VMEM((n_all, 1, lanes), f32),
            pltpu.VMEM((9, 16, lanes), f32), rows(16), rows(16), tiles(COMPS), tiles(2 * MAT),
            pltpu.SMEM((nshift,), f32), pltpu.SMEM((nshift,), f32), pltpu.SMEM((1,), f32), dma((5,)),
            dma((8,)), dma((8,)), dma((2,)), dma((2, 2)), dma((2,)), dma((2,)), dma((2,)), dma((2,)),
            pltpu.SemaphoreType.REGULAR,
        ],
        compiler_params=pltpu.CompilerParams(collective_id=0, has_side_effects=True),
    )(
        source.reshape(COMPS, 8, lanes), links.reshape(2 * MAT, 8, lanes), shifts, residues, mass
    )
    return rational.reshape(source.shape), action


def solution(mesh):
    sizes = tuple(mesh.shape[name] for name in ("grp", "zt", "xy"))
    field = P("grp", None, None, "xy", "zt", None)
    return jax.shard_map(
        functools.partial(on_device, sizes),
        mesh=mesh,
        in_specs=(field, P("grp", None, None, None, "xy", "zt", None), P(), P(), P()),
        out_specs=(field, P()),
        check_vma=False,
    )
```

```python
import functools

import jax
import jax.numpy as jnp
from jax import lax
from jax.experimental import pallas as pl
from jax.experimental.pallas import tpu as pltpu
from jax.sharding import PartitionSpec as P

NY = 2
NZ = 64
ITERS = 8
PAIRS = 9
MAT = 2 * PAIRS
COMPS = 6


def roll(value, shift, axis):
    size = value.shape[axis]
    return pltpu.roll(value, shift % size, axis)


def kernel(
    dims, source_hbm, links_hbm, shifts_hbm, residues_hbm, mass_hbm, out_ref, action_ref,
    lk, tfar, xfar, xtwo, sx, st, sx2, cs_ll, cs_hl, cs_lh, c_ll, c_hl, c_lh,
    gauge, wide, hop_w, hop_r, mid, dpack_ref, shiftdirs, rpack, ws, cs, hb, part, cross,
    state, mine, theirs, source_ref, links_ref, shifts_ref, residues_ref, mass_ref,
    isem, lsend, lrecv, hsend, hrecv, psend, precv, asend, arecv, ready,
):
    n_grp, n_zt, n_xy, cells_x, cells_t = dims
    lanes = NY * NZ
    n_all = n_zt * n_xy
    nshift = shifts_ref.shape[0]
    g = lax.axis_index("grp")
    zt = lax.axis_index("zt")
    xy = lax.axis_index("xy")
    me = zt * n_xy + xy
    me_all = g * n_all + me
    x_up, x_dn = lax.rem(xy + 1, n_xy), lax.rem(xy + n_xy - 1, n_xy)
    t_up, t_dn = lax.rem(zt + 1, n_zt), lax.rem(zt + n_zt - 1, n_zt)
    other = 1 - g

    def place(linear):
        inside = lax.rem(linear, n_all)
        return (linear // n_all, inside // n_xy, lax.rem(inside, n_xy))

    def each(count, fn):
        if count <= 32:
            for p in range(1, count):
                fn(p)
        else:
            def step(p, carry):
                fn(p)
                return carry
            lax.fori_loop(1, count, step, 0)

    def copy(src, dst, send, recv, device):
        return pltpu.make_async_remote_copy(
            src_ref=src, dst_ref=dst, send_sem=send, recv_sem=recv,
            device_id=device, device_id_type=pl.DeviceIdType.MESH,
        )

    barrier = pltpu.get_barrier_semaphore()

    corner_dev = ((g, t_up, x_up), (g, t_dn, x_up), (g, t_up, x_dn), (g, t_dn, x_dn))
    above = ((g, zt, x_up),) + corner_dev[:2]
    partners = ((other, zt, xy), (g, t_up, xy), (g, t_dn, xy), (g, zt, x_dn)) + corner_dev[2:]
    near_barrier = n_zt <= 4 and n_xy <= 4
    at_top, at_bottom = xy == n_xy - 1, xy == 0

    def greet(device):
        pl.semaphore_signal(barrier, inc=1, device_id=device, device_id_type=pl.DeviceIdType.MESH)

    fetch_links = pltpu.make_async_copy(links_hbm, links_ref, isem.at[0])
    fetch_source = pltpu.make_async_copy(source_hbm, source_ref, isem.at[1])
    if near_barrier:
        for device in partners:
            greet(device)

        @pl.when(jnp.logical_not(at_top))
        def _():
            for device in above:
                greet(device)
    else:
        each(n_grp * n_all, lambda p: greet(place(lax.rem(me_all + p, n_grp * n_all))))
    fetch_links.start()
    fetch_source.start()
    scalars = [
        pltpu.make_async_copy(src, dst, isem.at[2 + k])
        for k, (src, dst) in enumerate(((shifts_hbm, shifts_ref), (residues_hbm, residues_ref), (mass_hbm, mass_ref)))
    ]
    for item in scalars:
        item.start()
    fetch_links.wait()
    fetch_source.wait()

    sub = lax.broadcasted_iota(jnp.int32, (8, lanes), 0)
    lane = lax.broadcasted_iota(jnp.int32, (8, lanes), 1)
    zcoord = lax.rem(lane, NZ)
    ycoord = lane // NZ
    quarter = lanes // 4
    home = sub == lane // quarter
    own = (sub >= 2) & (sub < 2 + cells_t)
    first = sub < cells_t
    late = lax.rem(sub, cells_t) >= 2

    def t_faces(c, one, two):
        st[0, pl.ds(c, 1)] = jnp.where(late, one, roll(two, -2, 0))[None]
        st[1, pl.ds(c, 1)] = jnp.where(late, roll(two, 2, 0), one)[None]

    for d in range(2):
        for c in range(MAT):
            low, high = links_ref[c], links_ref[MAT + c]
            if d == 0:
                sx[0, pl.ds(g * MAT + c, 1)] = jnp.where(first, roll(low, 4, 0), high)[None]
            else:
                sx[1, pl.ds(g * MAT + c, 1)] = jnp.where(first, low, roll(high, 4, 0))[None]
    for c in range(MAT):
        t_faces(g * MAT + c, links_ref[c], links_ref[MAT + c])
    for c in range(2 * MAT):
        lk[pl.ds(g * 2 * MAT + c, 1)] = links_ref[c][None]

    spack = [source_ref[c] for c in range(COMPS)]

    def corner_tiles(tiles, par):
        for k, row in enumerate((7, 4, 3, 0)):
            tile = jnp.zeros((8, lanes), jnp.float32)
            for c in range(COMPS):
                tile = jnp.where(sub == c, jnp.broadcast_to(tiles[c][row:row + 1], (8, lanes)), tile)
            cs[par, k] = tile

    def face(par, k):
        device = ((g, zt, x_up), (g, zt, x_dn), (g, t_up, xy), (g, t_dn, xy))[k]
        at = k * COMPS if k < 2 else k * COMPS + 4
        return copy(ws.at[par], hb.at[par, pl.ds(at, COMPS)], hsend.at[par], hrecv.at[par, k // 2], device)

    def corner(par, k):
        return copy(cs.at[par, pl.ds(k, 1)], hb.at[par, pl.ds(2 * COMPS + k, 1)], hsend.at[par], hrecv.at[par, 0], corner_dev[k])

    def start_faces(par):
        face(par, 2).start()
        face(par, 3).start()

        @pl.when(at_bottom)
        def _():
            face(par, 1).start()
        face(par, 0).start()

        @pl.when(jnp.logical_not(at_bottom))
        def _():
            face(par, 1).start()

    def start_corners(par):
        for k in range(4):
            corner(par, k).start()

    def send_part(par):
        def go(p):
            copy(part.at[par, me], part.at[par, me], psend.at[par], precv.at[par],
                 (g,) + place(lax.rem(me + p, n_all))[1:]).start()
        each(n_all, go)

    def wait_part(par):
        rest = part.at[par, pl.ds(0, n_all - 1)]
        copy(rest, rest, psend.at[par], precv.at[par], corner_dev[0]).wait()

    def send_cross(par):
        def go(p):
            copy(part.at[par, me], cross.at[me], asend.at[0], arecv.at[0],
                 (other,) + place(lax.rem(me + p, n_all))[1:]).start()
        go(0)
        each(n_all, go)

    def dots(rows):
        tile = jnp.zeros((8, lanes), jnp.float32)
        for k, row in enumerate(rows):
            tile = jnp.where(sub == k, jnp.broadcast_to(jnp.sum(row, axis=0, keepdims=True), (8, lanes)), tile)
        tile = (tile + roll(tile, 2 * quarter, 1)) + (roll(tile, quarter, 1) + roll(tile, 3 * quarter, 1))
        return jnp.sum(jnp.where(home, tile, 0.0), axis=0, keepdims=True)

    def summed(row_of):
        if n_all <= 32:
            level = [row_of(j) for j in range(n_all)]
            while len(level) > 1:
                odd = level[len(level) // 2 * 2:]
                level = [level[k] + level[k + 1] for k in range(0, len(level) - 1, 2)] + odd
            total = level[0]
        else:
            total = lax.fori_loop(1, n_all, lambda j, acc: acc + row_of(j), row_of(0))
        split = jnp.where(home, jnp.broadcast_to(total, (8, lanes)), 0.0)
        return jnp.broadcast_to(jnp.sum(split, axis=1, keepdims=True), (8, lanes))

    def fill(values, k):
        return jnp.broadcast_to(values[k:k + 1], (16, lanes))

    def inner(left, right):
        total = left[0] * right[0]
        for c in range(1, COMPS):
            total = total + left[c] * right[c]
        return total

    corner_tiles(spack, 0)
    for c in range(COMPS):
        ws[0, c] = spack[c]

    if near_barrier:
        pl.semaphore_wait(barrier, len(partners) + jnp.where(at_bottom, 0, len(above)))

        @pl.when(at_top)
        def _():
            for device in above:
                pl.semaphore_signal(ready, inc=1, device_id=device, device_id_type=pl.DeviceIdType.MESH)
    else:
        pl.semaphore_wait(barrier, n_grp * n_all - 1)

    half = 2 * MAT

    def to_pair(k):
        found = []
        for d in range(2):
            span = d * MAT + k * PAIRS
            found.append(copy(
                links_ref.at[pl.ds(span, PAIRS)], lk.at[pl.ds(g * half + span, PAIRS)],
                lsend.at[k], lrecv.at[k], (other, zt, xy),
            ))
        return found

    def span_of(h, k):
        return pl.ds(h * MAT + k * PAIRS, PAIRS)

    def up_face(h, k):
        span = span_of(h, k)
        return copy(sx.at[0, span], xfar.at[0, span], lsend.at[2], lrecv.at[2], (g, zt, x_up))

    def down_face(h, k):
        span = span_of(h, k)
        return copy(sx.at[1, span], xfar.at[1, span], lsend.at[2], lrecv.at[2], (g, zt, x_dn))

    def t_copies(h, k):
        span = span_of(h, k)
        return [
            copy(st.at[0, span], tfar.at[0, span], lsend.at[3], lrecv.at[3], (g, t_up, xy)),
            copy(st.at[1, span], tfar.at[1, span], lsend.at[3], lrecv.at[3], (g, t_dn, xy)),
        ]

    def below_near():
        for k in range(2):
            down_face(g, k).start()
        for k in (2, 3):
            corner(0, k).start()
        face(0, 1).start()

    for k in range(2):
        for item in to_pair(k):
            item.start()
    for k in range(2):
        for item in [up_face(g, k)] + t_copies(g, k):
            item.start()
    for k in (0, 1):
        corner(0, k).start()
    for k in (0, 2, 3):
        face(0, k).start()

    @pl.when(jnp.logical_not(at_bottom))
    def _():
        below_near()

    def pair_part(k):
        block = lk.at[pl.ds(k * MAT, MAT)]
        return copy(block, block, lsend.at[k], lrecv.at[k], (other, zt, xy))

    for k in range(2):
        pair_part(k).wait_recv()
        for c in range(k * PAIRS, (k + 1) * PAIRS):
            low, high = lk[other * half + c], lk[other * half + MAT + c]
            sx[0, pl.ds(other * MAT + c, 1)] = jnp.where(first, roll(low, 4, 0), high)[None]
            sx[1, pl.ds(other * MAT + c, 1)] = jnp.where(first, low, roll(high, 4, 0))[None]
            t_faces(other * MAT + c, low, high)
        for item in [up_face(other, k)] + t_copies(other, k):
            item.start()
        if k == 0:
            @pl.when(jnp.logical_not(at_bottom))
            def _():
                down_face(other, 0).start()
    for c in range(PAIRS):
        sx2[c] = jnp.where(first, lk[c], roll(lk[PAIRS + c], 4, 0))
    for c in range(MAT):
        cs_ll[c:c + 1] = lk[c][7:8]
        cs_ll[MAT + c:MAT + c + 1] = lk[3 * MAT + c][7:8]
        cs_hl[c:c + 1] = lk[3 * MAT + c][3:4]
        cs_lh[c:c + 1] = lk[c][4:5]
    rest = [
        copy(sx2, xtwo, lsend.at[4], lrecv.at[4], (g, zt, x_up)),
        copy(cs_ll, c_ll, lsend.at[5], lrecv.at[5], corner_dev[0]),
        copy(cs_lh, c_lh, lsend.at[6], lrecv.at[6], corner_dev[1]),
        copy(cs_hl, c_hl, lsend.at[7], lrecv.at[7], corner_dev[2]),
    ]
    for item in rest[:3]:
        item.start()

    @pl.when(at_bottom)
    def _():
        if near_barrier:
            pl.semaphore_wait(ready, len(above))
        below_near()
        down_face(other, 0).start()
    down_face(other, 1).start()
    rest[3].start()

    def pick(ref, c):
        return jnp.broadcast_to(ref[c:c + 1], (8, lanes))

    def widen(c, x, mine, low, high):
        between = jnp.where(late, low, high)
        return jnp.where(own, roll(mine, 2 - 4 * x, 0), roll(between, 6 - 4 * x, 0))

    def far_rows(block, low_corner, high_corner, x):
        row = jnp.where(own, roll(block, 2 - 4 * x, 0), 0.0)
        if low_corner is not None:
            row = jnp.where(sub == 1, low_corner, row)
        if high_corner is not None:
            row = jnp.where(sub == 6, high_corner, row)
        return row

    def extend_t(par, c):
        t_lo, t_hi = hb[par, 2 * COMPS + 4 + c], hb[par, 3 * COMPS + 4 + c]
        for x in range(2):
            wide[c, 2 + x] = widen(c, x, ws[par, c], t_lo, t_hi)

    def extend_x(par, c):
        corners = [jnp.broadcast_to(hb[par, 2 * COMPS + k, c:c + 1], (8, lanes)) for k in range(4)]
        x_lo, x_hi = hb[par, c], hb[par, COMPS + c]
        wide[c, 0] = far_rows(x_lo, None, None, 0)
        wide[c, 1] = far_rows(x_lo, corners[0], corners[1], 1)
        wide[c, 4] = far_rows(x_hi, corners[2], corners[3], 0)
        wide[c, 5] = far_rows(x_hi, None, None, 1)

    for item in scalars:
        item.wait()
    rows16 = lax.broadcasted_iota(jnp.int32, (16, lanes), 0)
    shift_rows = jnp.zeros((16, lanes), jnp.float32)
    residue_rows = jnp.zeros((16, lanes), jnp.float32)
    for k in range(nshift):
        shift_rows = jnp.where(rows16 == k, shifts_ref[k], shift_rows)
        residue_rows = jnp.where(rows16 == k, residues_ref[k], residue_rows)
    mass_sq = mass_ref[0] * mass_ref[0]

    for c in range(COMPS):
        rpack[c] = spack[c]
        out_ref[c] = jnp.zeros((8, lanes), jnp.float32)
        for k in range(nshift):
            shiftdirs[k, c] = spack[c]

    copy(st, tfar, lsend.at[3], lrecv.at[3], (g, t_up, xy)).wait()
    for k in range(2):
        pair_part(k).wait_send()

    t_at = lax.rem(zt * cells_t + sub - 2 + n_zt * cells_t, n_zt * cells_t)
    edge = jnp.where(t_at == n_zt * cells_t - 1, -0.5, 0.5)
    yz_sign = (1 - 2 * lax.rem(ycoord + zcoord, 2)).astype(jnp.float32)
    y_sign = (1 - 2 * lax.rem(ycoord, 2)).astype(jnp.float32)

    def z_up(v):
        cond = jnp.broadcast_to(zcoord == NZ - 1, v.shape)
        return jnp.where(cond, roll(v, NZ - 1, v.ndim - 1), roll(v, -1, v.ndim - 1))

    def z_dn(v):
        cond = jnp.broadcast_to(zcoord == 0, v.shape)
        return jnp.where(cond, roll(v, 1 - NZ, v.ndim - 1), roll(v, 1, v.ndim - 1))

    def wide_link(d, c, e):
        at = d * MAT + c
        sign = -1.0 if e % 2 else 1.0
        if e in (2, 3):
            low, high = tfar[0, (d // 2) * MAT + c], tfar[1, (d // 2) * MAT + c]
            if d % 2:
                low, high = roll(low, 2, 0), roll(high, -2, 0)
            value = widen(c, e - 2, lk[at], low, high)
        elif e == 0:
            value = far_rows(xtwo[c % PAIRS], None, None, c // PAIRS)
        elif e == 1:
            low = pick(c_ll, c) if d == 0 else (pick(c_ll, MAT + c) if d == 3 else None)
            value = far_rows(xfar[0, (d // 2) * MAT + c], low, pick(c_lh, c) if d == 0 else None, d % 2)
        else:
            value = far_rows(xfar[1, (d // 2) * MAT + c], pick(c_hl, c) if d == 3 else None, None, d % 2)
        if d == 0:
            return 0.5 * value
        if d == 1:
            return (0.5 * sign) * value
        if d == 2:
            return (0.5 * sign) * y_sign * value
        return sign * yz_sign * edge * value

    def build(rows):
        for part_no in range(2):
            for i in range(3):
                for j in range(3):
                    c = part_no * PAIRS + i * 3 + j
                    flip = part_no * PAIRS + j * 3 + i
                    back = 1.0 if part_no else -1.0
                    for e in rows:
                        wx = wide_link(0, c, e)
                        if e > 0:
                            gauge[0, c, e - 1] = wx
                        if e < 4:
                            gauge[1, flip, e] = back * wx
                        if e == 0:
                            continue
                        wz = wide_link(2, c, e)
                        gauge[3, c, e - 1] = wz
                        gauge[4, flip, e - 1] = back * z_dn(wz)
                        wt = wide_link(3, c, e)
                        gauge[5, c, e - 1] = wt
                        gauge[6, flip, e - 1] = back * roll(wt, 1, 0)
                        wy = wide_link(1, c, e)
                        turned = wide_link(1, flip, e)
                        gauge[2, c, e - 1] = wy + back * roll(turned, NZ, 1)

    build((2, 3))
    for item in [copy(sx, xfar, lsend.at[2], lrecv.at[2], (g, zt, x_up))] + rest:
        item.wait()
    build((0, 1, 4))

    def wait_x(par):
        block = hb.at[par, pl.ds(0, 2 * COMPS + 4)]
        copy(block, block, hsend.at[par], hrecv.at[par, 0], corner_dev[0]).wait_recv()

    def wait_t(par):
        block = hb.at[par, pl.ds(2 * COMPS + 4, 2 * COMPS)]
        copy(block, block, hsend.at[par], hrecv.at[par, 1], corner_dev[0]).wait_recv()

    def wait_sent(par):
        copy(hb.at[par], hb.at[par], hsend.at[par], hrecv.at[par, 0], corner_dev[0]).wait_send()

    def hop(field, e0, count, terms, total):
        shifts_of = (
            lambda c: field[c, e0 + 1:e0 + 1 + count],
            lambda c: field[c, e0 - 1:e0 - 1 + count],
            lambda c: roll(field[c, e0:e0 + count], NZ, 2),
            lambda c: z_up(field[c, e0:e0 + count]),
            lambda c: z_dn(field[c, e0:e0 + count]),
            lambda c: roll(field[c, e0:e0 + count], -1, 1),
            lambda c: roll(field[c, e0:e0 + count], 1, 1),
        )
        for term in terms:
            v = [shifts_of[term](c) for c in range(COMPS)]
            for i in range(3):
                for j in range(3):
                    wre = gauge[term, i * 3 + j, e0 - 1:e0 - 1 + count]
                    wim = gauge[term, PAIRS + i * 3 + j, e0 - 1:e0 - 1 + count]
                    re = wre * v[j] - wim * v[3 + j]
                    im = wre * v[3 + j] + wim * v[j]
                    total[i] = re if total[i] is None else total[i] + re
                    total[3 + i] = im if total[3 + i] is None else total[3 + i] + im
        return total

    every = tuple(range(7))

    def hop_wide(par):
        wait_t(par)
        for c in range(COMPS):
            extend_t(par, c)
        for c, value in enumerate(hop(wide, 2, 2, every[2:], [None] * COMPS)):
            hop_w[c, 2:4] = value
        wait_x(par)
        for c in range(COMPS):
            extend_x(par, c)
        for c, value in enumerate(hop(wide, 2, 2, every[:2], [hop_w[c, 2:4] for c in range(COMPS)])):
            hop_w[c, 2:4] = value
        for e in (1, 4):
            for c, value in enumerate(hop(wide, e, 1, every, [None] * COMPS)):
                hop_w[c, e:e + 1] = value
        wait_sent(par)

    hop_wide(0)
    for c in range(COMPS):
        dpack_ref[c] = spack[c]
        hop_r[c, 1:5] = hop_w[c, 1:5]
        mid[c, 1:5] = hop_w[c, 1:5]

    def image_of():
        image = hop(mid, 2, 2, every, [None] * COMPS)
        packed = []
        for c in range(COMPS):
            wp = jnp.where(first, roll(image[c][0], -2, 0), roll(image[c][1], 2, 0))
            packed.append(mass_sq * dpack_ref[c] - wp)
        return packed, [dpack_ref[c] for c in range(COMPS)]

    def row(values, k):
        return jnp.broadcast_to(values[k:k + 1], (8, lanes))

    def accumulate(gain):
        for c in range(COMPS):
            total = out_ref[c]
            for k in range(nshift):
                total = total + row(gain, k) * shiftdirs[k, c]
            out_ref[c] = total

    def catch_up(gain, zeta_now, beta_shift):
        accumulate(gain)
        for k in range(nshift):
            zk, bk = row(zeta_now, k), row(beta_shift, k)
            for c in range(COMPS):
                shiftdirs[k, c] = zk * rpack[c] + bk * shiftdirs[k, c]

    lane16 = lax.broadcasted_iota(jnp.int32, (16, lanes), 1)
    swap = copy(mine, theirs, asend.at[1], arecv.at[1], (other, zt, xy))

    def closing(sums, values):
        norm, zeta, zeta_old, alpha_old, beta_old, beta_shift, along, score = values
        alpha = norm / fill(sums, 0)
        zeta_new = zeta * zeta_old * alpha_old / (
            alpha * beta_old * (zeta_old - zeta) + zeta_old * alpha_old * (1.0 + shift_rows * alpha)
        )
        gain = residue_rows * alpha * (zeta_new / zeta)
        return gain, score + gain * (zeta * fill(sums, 3) + beta_shift * along)

    def iterate(step, last):
        norm, zeta, zeta_old, alpha_old, beta_old, beta_shift, along, score, gain = [state[k] for k in range(9)]
        par = step % 2 if last else lax.rem(step, 2)
        if last:
            packed_state = norm
            for k in range(1, 8):
                packed_state = jnp.where(lane16 == k, state[k], packed_state)
            mine[...] = packed_state
            swap.start()
        packed, dpack = image_of()
        res = [rpack[c] for c in range(COMPS)]
        sums_row = dots([inner(dpack, packed), inner(res, packed), inner(packed, packed), inner(spack, res)])
        if not last:
            corner_tiles(packed, par)
            for c in range(COMPS):
                ws[par, c] = packed[c]
            start_corners(par)
        part[par, pl.ds(me, 1)] = sums_row[None]
        send_part(par)
        if last:
            send_cross(par)
        else:
            start_faces(par)
        catch_up(gain, zeta, beta_shift)
        if not last:
            hop_wide(par)
        wait_part(par)
        sums = summed(lambda j: part[par, j])
        if last:
            gain, score = closing(sums, [state[k] for k in range(8)])
            accumulate(gain)
            return score
        norm = jnp.where(step == 1, fill(sums, 3), norm)
        alpha = norm / fill(sums, 0)
        zeta_new = zeta * zeta_old * alpha_old / (
            alpha * beta_old * (zeta_old - zeta) + zeta_old * alpha_old * (1.0 + shift_rows * alpha)
        )
        ratio = zeta_new / zeta
        along = zeta * fill(sums, 3) + beta_shift * along
        gain = residue_rows * alpha * ratio
        score = score + gain * along
        norm_next = norm - 2.0 * alpha * fill(sums, 1) + alpha * alpha * fill(sums, 2)
        beta = norm_next / norm
        beta_shift = beta * ratio * ratio
        step_a, step_b = row(alpha, 0), row(beta, 0)
        for c in range(COMPS):
            fresh = rpack[c] - step_a * ws[par, c]
            rpack[c] = fresh
            dpack_ref[c] = fresh + step_b * dpack_ref[c]
            for e in range(1, 5):
                fresh = hop_r[c, e] - step_a * hop_w[c, e]
                hop_r[c, e] = fresh
                mid[c, e] = fresh + step_b * mid[c, e]
        for k, value in enumerate((norm_next, zeta_new, zeta, alpha, beta, beta_shift, along, score, gain)):
            state[k] = value

    one = jnp.ones((16, lanes), jnp.float32)
    none = jnp.zeros((16, lanes), jnp.float32)

    def body(step, carry):
        iterate(step, False)
        return carry

    for k, value in enumerate((one, one, one, one, none, none, none, none, none)):
        state[k] = value
    lax.fori_loop(1, ITERS, body, 0)
    score = iterate(ITERS, True)
    swap.wait()
    copy(cross, cross, asend.at[0], arecv.at[0], corner_dev[0]).wait()
    far_state = theirs[...]
    values = [jnp.broadcast_to(far_state[:, k:k + 1], (16, lanes)) for k in range(8)]
    total = score + closing(summed(lambda j: cross[j]), values)[1]
    sites = n_grp * n_all * cells_x * cells_t * lanes
    action_ref[0] = jnp.max(jnp.sum(total, axis=0, keepdims=True)) * (1.0 / sites)


def on_device(sizes, source, links, shifts, residues, mass):
    n_grp, n_zt, n_xy = sizes
    cells_x, cells_t, lanes = source.shape[3:]
    n_all = n_zt * n_xy
    f32 = jnp.float32
    tiles = lambda *lead: pltpu.VMEM(lead + (8, lanes), f32)
    rows = lambda count: pltpu.VMEM((count, lanes), f32)
    nshift = shifts.shape[0]
    vmem = pl.BlockSpec(memory_space=pltpu.VMEM)
    smem = pl.BlockSpec(memory_space=pltpu.SMEM)
    dma = pltpu.SemaphoreType.DMA
    rational, action = pl.pallas_call(
        functools.partial(kernel, (n_grp, n_zt, n_xy, cells_x, cells_t)),
        out_shape=(
            pltpu.VMEM((COMPS, 8, lanes), f32),
            pltpu.SMEM((1,), f32),
        ),
        in_specs=[pl.BlockSpec(memory_space=pltpu.HBM)] * 5,
        out_specs=(vmem, smem),
        scratch_shapes=[
            tiles(4 * MAT), tiles(2, 2 * MAT), tiles(2, 2 * MAT), tiles(PAIRS), tiles(2, 2 * MAT), tiles(2, 2 * MAT), tiles(PAIRS),
            rows(40), rows(24), rows(24), rows(40), rows(24), rows(24),
            tiles(7, MAT, 4), tiles(COMPS, 6), tiles(COMPS, 6), tiles(COMPS, 6), tiles(COMPS, 6), tiles(COMPS),
            tiles(nshift, COMPS), tiles(COMPS), tiles(2, COMPS), tiles(2, 4), tiles(2, 4 * COMPS + 4),
            pltpu.VMEM((2, n_all, 1, lanes), f32), pltpu.VMEM((n_all, 1, lanes), f32),
            pltpu.VMEM((9, 16, lanes), f32), rows(16), rows(16), tiles(COMPS), tiles(2 * MAT),
            pltpu.SMEM((nshift,), f32), pltpu.SMEM((nshift,), f32), pltpu.SMEM((1,), f32), dma((5,)),
            dma((8,)), dma((8,)), dma((2,)), dma((2, 2)), dma((2,)), dma((2,)), dma((2,)), dma((2,)),
            pltpu.SemaphoreType.REGULAR,
        ],
        compiler_params=pltpu.CompilerParams(collective_id=0, has_side_effects=True),
    )(
        source.reshape(COMPS, 8, lanes), links.reshape(2 * MAT, 8, lanes), shifts, residues, mass
    )
    return rational.reshape(source.shape), action


def solution(mesh):
    sizes = tuple(mesh.shape[name] for name in ("grp", "zt", "xy"))
    field = P("grp", None, None, "xy", "zt", None)
    return jax.shard_map(
        functools.partial(on_device, sizes),
        mesh=mesh,
        in_specs=(field, P("grp", None, None, None, "xy", "zt", None), P(), P(), P()),
        out_specs=(field, P()),
        check_vma=False,
    )
```
